512 devices in a mesh: lat: 16 (over y, x_lo, core), lon: 32 (over x_hi, z).
Axes of the slice: x: 4 (x_hi: 2, x_lo: 2; x = x_hi * 2 + x_lo), y: 4, z: 16, core: 2. Of those that a mesh axis runs over, the one named last changes fastest.
Arguments:
- ensemble: bfloat16 [128, 512, 2048], P('lat', 'lon'), may hold values from -6 to 6
- channel_weights: bfloat16 [16, 32, 32, 32, 128], P('lat', 'lon'), may hold values from -1 to 1
- block_column: int32 [16, 32, 32], P('lat', 'lon'), may hold values from 0 to 127
- innovation: bfloat16 [16, 32, 32, 128], P('lat', 'lon'), may hold values from -6 to 6
- error_precision: bfloat16 [16, 32, 32, 128], P('lat', 'lon'), may hold values from 0.25 to 4
- block_count: int32 [16, 32], P('lat', 'lon'), may hold values from 1 to 32, as said below
- neighbours: int32 [64, 256, 12], P('lat', 'lon'), may hold values from 0 to 287
Outputs:
- analysis: bfloat16 [128, 512, 2048], P('lat', 'lon')
The draws below stay inside these ranges and needn't reach their ends.
Inputs may be any that keep to these rules, and one draw needn't show every extreme that they name: The live blocks of a tile are its first block_count slots; at least one tile fills all 32 slots.
All inputs are finite; a program needn't handle non-finite values.
Results may differ from the reference program's by a relative error of at most 0.0074.
Values may be sent and summed in bfloat16 or wider, within the bound.
A program may use at most 64 MiB of HBM per device.

```python
import math
import jax
import jax.numpy as jnp
from jax import lax

K = 64
L = 32
OB = 128
CLAT = 8
CLON = 16
NBLK = 32
NNB = 12
NSI = 6
NLAT = 128
NLON = 512
TLAT = 16
TLON = 32
GLAT = 64
GLON = 256
LOC = 12


def draw_block_count(key, part):
    raw_draw = jax.random.randint(key, (TLAT, TLON), 1, NBLK + 1)
    counts = jnp.maximum(1, raw_draw * raw_draw // NBLK)
    chosen = jax.random.randint(jax.random.fold_in(key, 7), (), 0, TLAT * TLON)
    counts = counts.reshape(-1).at[chosen].set(NBLK).reshape(TLAT, TLON)
    return counts.astype(jnp.int32)


def with_ends(drawn, own_key, smallest, top_value):
    longest = drawn.shape.index(max(drawn.shape))
    spots = []
    for shift in (0, 1):
        where = [jax.random.randint(jax.random.fold_in(own_key, axis), (), 0, length) for axis, length in enumerate(drawn.shape)]
        where[longest] = (where[longest] + shift) % drawn.shape[longest]
        spots.append(tuple(where))
    return drawn.at[spots[0]].set(smallest).at[spots[1]].set(top_value)


def levels(key, shape, shards, smallest, largest):
    factor_of, own = 1.0, jax.random.fold_in(key, 6)
    for dim, blocks in shards:
        draws = jnp.exp(jax.random.uniform(jax.random.fold_in(own, dim), (blocks,), jnp.float32, smallest / len(shards), largest / len(shards)))
        factor_of = factor_of * jnp.repeat(draws, shape[dim] // blocks).reshape([-1 if axis == dim else 1 for axis in range(len(shape))])
    return factor_of


def gaussian(stream_key, dims, width, most, cuts=(), held_as=jnp.bfloat16):
    level = levels(stream_key, dims, cuts, -0.22, 0.18) if cuts else 1.0
    values = jax.random.normal(stream_key, dims, jnp.float32) * width * level
    return jnp.minimum(jnp.maximum(values, -most), most).astype(held_as)


def setup_inputs(seed: int = 0) -> dict:
    key_of = jax.random.split(jax.random.key(seed), 8)
    ensemble = gaussian(key_of[0], (NLAT, NLON, L * K), 1.0, 6.0, ((0, 16), (1, 32)))
    channel_weights = gaussian(key_of[1], (TLAT, TLON, NBLK, L, OB), L ** -0.5, 1.0, ((0, 16), (1, 32)))
    block_column = with_ends(jax.random.randint(key_of[2], (TLAT, TLON, NBLK), 0, CLAT * CLON), jax.random.fold_in(key_of[2], 1), 0, (CLAT * CLON) - 1).astype(jnp.int32)
    innovation = gaussian(key_of[3], (TLAT, TLON, NBLK, OB), 1.0, 6.0, ((0, 16), (1, 32)))
    error_precision = jnp.clip(jnp.exp(math.log(4.0) - 2.7725887 * jax.random.uniform(key_of[4], (TLAT, TLON, NBLK, OB), jnp.float32) ** levels(key_of[4], (TLAT, TLON, NBLK, OB), ((0, 16), (1, 32)), -0.2, 0.2)), 0.25, 4.0).astype(jnp.bfloat16)
    block_count = draw_block_count(jax.random.fold_in(key_of[7], 71), 0)
    neighbours = with_ends(jax.random.randint(key_of[6], (GLAT, GLON, NNB), 0, 9 * NBLK), jax.random.fold_in(key_of[6], 1), 0, (9 * NBLK) - 1).astype(jnp.int32)
    return {"ensemble": ensemble, "channel_weights": channel_weights, "block_column": block_column, "innovation": innovation, "error_precision": error_precision, "block_count": block_count, "neighbours": neighbours}


def newton_schulz(gram_matrix, projected):
    members = gram_matrix.shape[-1]
    identity = jnp.eye(members, dtype=jnp.float32)
    frobenius = jnp.sqrt(lax.optimization_barrier(jnp.sum(gram_matrix * gram_matrix, axis=(1, 2))))
    current = gram_matrix / frobenius[:, None, None]
    inverse = jnp.broadcast_to(identity, gram_matrix.shape)
    for turn_index in range(NSI):
        middle = 1.5 * identity - 0.5 * jnp.einsum('pij,pjk->pik', inverse, current, precision=lax.Precision.HIGHEST)
        current = jnp.einsum('pij,pjk->pik', current, middle, precision=lax.Precision.HIGHEST)
        inverse = jnp.einsum('pij,pjk->pik', middle, inverse, precision=lax.Precision.HIGHEST)
    root_scale = jnp.sqrt(frobenius)
    spread_part = inverse * (jnp.sqrt(jnp.float32(members - 1.0)) / root_scale)[:, None, None]
    halfway = jnp.einsum('pij,pj->pi', inverse, projected, precision=lax.Precision.HIGHEST)
    mean_shift = jnp.einsum('pij,pj->pi', inverse, halfway, precision=lax.Precision.HIGHEST) / frobenius[:, None]
    return (spread_part + mean_shift[:, :, None]).astype(jnp.bfloat16)

def reference(ensemble, channel_weights, block_column, innovation, error_precision, block_count, neighbours):
    half_lat = CLAT // 2
    half_lon = CLON // 2
    innovation_wide = innovation.astype(jnp.float32)
    precision_wide = error_precision.astype(jnp.float32)
    tile_lat = jnp.arange(TLAT, dtype=jnp.int32)[:, None, None]
    tile_lon = jnp.arange(TLON, dtype=jnp.int32)[None, :, None]
    glob_lat = tile_lat * CLAT + block_column // CLON
    glob_lon = tile_lon * CLON + block_column % CLON
    picked = ensemble[glob_lat, glob_lon].reshape(TLAT, TLON, NBLK, L, K).astype(jnp.float32)
    average = lax.optimization_barrier(jnp.mean(picked, axis=4, keepdims=True))
    anomaly = (picked - average).astype(jnp.bfloat16)
    blocks = jnp.einsum('abdlk,abdlo->abdko', anomaly.astype(jnp.float32), channel_weights.astype(jnp.float32), precision=lax.Precision.HIGHEST).astype(jnp.bfloat16)

    def coarse_row(row_index):
        tile_row = row_index // half_lat
        local_row = row_index % half_lat
        listed = neighbours[row_index]
        point_lon = jnp.arange(GLON, dtype=jnp.int32)
        tile_col = (point_lon // half_lon)[:, None]
        local_col = (point_lon % half_lon)[:, None]
        offset = listed // NBLK
        slot_index = listed % NBLK
        step_lat = offset // 3 - 1
        step_lon = offset % 3 - 1
        source_lat = tile_row + step_lat
        valid = (source_lat >= 0) & (source_lat < TLAT)
        source_lat = jnp.clip(source_lat, 0, TLAT - 1)
        source_lon = (tile_col + step_lon) % TLON
        column = block_column[source_lat, source_lon, slot_index]
        north_south = step_lat.astype(jnp.float32) * CLAT + (column // CLON).astype(jnp.float32)
        east_west = step_lon.astype(jnp.float32) * CLON + (column % CLON).astype(jnp.float32)
        delta_lat = north_south - 2.0 * local_row.astype(jnp.float32)
        delta_lon = east_west - 2.0 * local_col.astype(jnp.float32)
        taper = jnp.exp(-(delta_lat * delta_lat + delta_lon * delta_lon) / (2.0 * LOC * LOC))
        live_mask = (valid & (slot_index < block_count[source_lat, source_lon])).astype(jnp.float32)
        weighted = precision_wide[source_lat, source_lon, slot_index] * live_mask[:, :, None]
        root_weight = jnp.sqrt(taper[:, :, None] * weighted)
        chosen = blocks[source_lat, source_lon, slot_index]
        scaled = (root_weight[:, :, None, :] * chosen.astype(jnp.float32)).astype(jnp.bfloat16)
        forced = (root_weight * innovation_wide[source_lat, source_lon, slot_index]).astype(jnp.bfloat16)
        scaled_wide = scaled.astype(jnp.float32)
        gram_matrix = jnp.einsum('pjko,pjlo->pkl', scaled_wide, scaled_wide, precision=lax.Precision.HIGHEST) + (K - 1.0) * jnp.eye(K, dtype=jnp.float32)
        projected = jnp.einsum('pjko,pjo->pk', scaled_wide, forced.astype(jnp.float32), precision=lax.Precision.HIGHEST)
        return newton_schulz(gram_matrix, projected)
    coarse = lax.map(coarse_row, jnp.arange(GLAT, dtype=jnp.int32)).reshape(GLAT, GLON, K * K)
    coarse_ext = jnp.concatenate([coarse, coarse[-1:]], 0)
    coarse_ext = jnp.concatenate([coarse_ext, coarse_ext[:, :1]], 1)
    state_rows = ensemble.reshape(GLAT, 2, NLON, L * K)

    def fine_pair(pieces):
        upper, lower, pair_rows = pieces
        top_row = upper.astype(jnp.float32)
        bottom_row = lower.astype(jnp.float32)
        row_pair = jnp.stack([top_row, 0.5 * (top_row + bottom_row)], 0)
        col_even = row_pair[:, :-1]
        col_odd = 0.5 * (row_pair[:, :-1] + row_pair[:, 1:])
        blended = jnp.stack([col_even, col_odd], 2).reshape(2, NLON, K, K).astype(jnp.bfloat16)
        state_full = pair_rows.reshape(2, NLON, L, K).astype(jnp.float32)
        center = lax.optimization_barrier(jnp.mean(state_full, axis=3, keepdims=True))
        spread = (state_full - center).astype(jnp.bfloat16)
        result = center + jnp.einsum('rclk,rckj->rclj', spread.astype(jnp.float32), blended.astype(jnp.float32), precision=lax.Precision.HIGHEST)
        return result.astype(jnp.bfloat16).reshape(2, NLON, L * K)
    output = lax.map(fine_pair, (coarse_ext[:-1], coarse_ext[1:], state_rows))
    return output.reshape(NLAT, NLON, L * K)
```

```python
import functools

import jax
import jax.numpy as jnp
from jax import lax
from jax.experimental import pallas as pl
from jax.experimental.pallas import tpu as pltpu
from jax.sharding import PartitionSpec as P

F32 = jnp.float32
BF16 = jnp.bfloat16
MESH = pl.DeviceIdType.MESH
NSI = 6
LOC = 12
K = 64
OB = 128
CLAT = 8
CLON = 16
NBLK = 32
NNB = 12
LEV = 32
NT = 33
PAD = 33
CHUNKS = ((0, 11), (11, 22), (22, 33))


def dot(a, b):
    return jnp.dot(a, b, preferred_element_type=F32)


def split(x):
    hi = x.astype(BF16)
    return hi, (x - hi.astype(F32)).astype(BF16)


def diagonal(x, left, right):
    first, second = x[:, :128], x[:, 128:]
    zero = jnp.zeros_like(first)
    return jnp.concatenate(
        [
            jnp.concatenate([first * left, zero], 1),
            jnp.concatenate([first * right, zero], 1),
            jnp.concatenate([zero, second * left], 1),
            jnp.concatenate([zero, second * right], 1),
        ],
        0,
    )


def kernel(
    na, nb, ens, w, bcol, innov, prec, cnt, nbs, out,
    sa, sg, sp, gall, nbp, msend, mrecv, ssend, srecv, own, s2, yz, zf, tb, csend, rrow, rcol, rcor, dd, xa, sx, so,
    scales, g_send, g_recv, n_send, n_recv, m_send, m_recv, s_send, s_recv, t_send, t_recv,
):
    ia, jb = lax.axis_index("lat"), lax.axis_index("lon")
    up, down = lax.rem(ia + na - 1, na), lax.rem(ia + 1, na)
    west, east = lax.rem(jb + nb - 1, nb), lax.rem(jb + 1, nb)

    barrier = pltpu.get_barrier_semaphore()
    for peer in ((up, jb), (down, jb), (ia, west), (ia, east), (up, west), (down, east)):
        pl.semaphore_signal(barrier, inc=1, device_id=peer, device_id_type=MESH)

    def remote(src, dst, send, recv, peer):
        return pltpu.make_async_remote_copy(
            src_ref=src, dst_ref=dst, send_sem=send, recv_sem=recv, device_id=peer, device_id_type=MESH
        )

    lane1 = lax.broadcasted_iota(jnp.int32, (1, 128), 1)
    left_f = (lane1 < 64).astype(F32)
    left, right = left_f.astype(BF16), (1.0 - left_f).astype(BF16)
    row128 = lax.broadcasted_iota(jnp.int32, (128, 128), 0)
    lane128 = lax.broadcasted_iota(jnp.int32, (128, 128), 1)
    averager = jnp.where(row128 // 64 == lane128 // 64, 1.0 / K, 0.0).astype(BF16)

    code = jnp.zeros((1, 128), jnp.int32)
    columns = jnp.concatenate([bcol[...], jnp.zeros((1, 128 - NBLK), jnp.int32)], 1)
    live = (lane1 < cnt[0, 0]) & (lane1 < NBLK)
    code = jnp.where(live, columns + 1, 0)
    msend[0] = jnp.broadcast_to(code, (8, 128))
    msend[1] = jnp.broadcast_to(pltpu.roll(code, 2 * NBLK, 1), (8, 128))
    code_own = pltpu.roll(code, NBLK, 1)
    nbp[1, :, 0:NNB] = nbs[...]

    chosen = jnp.where(row128 == jnp.broadcast_to(columns, (128, 128)), 1.0, 0.0)
    chosen = jnp.where(lane128 < NBLK, chosen, 0.0)
    chosen = jnp.transpose(chosen)[:NBLK].astype(BF16)
    state = ens[...].reshape(CLAT * CLON, LEV * K)
    picked = dot(chosen, state)
    stacked = jnp.concatenate([picked[:, 128 * t : 128 * (t + 1)] for t in range(16)], 0)
    anomaly = stacked - dot(stacked.astype(BF16), averager)
    for t in range(16):
        part = anomaly[NBLK * t : NBLK * (t + 1)]
        sa[pl.ds(2 * t * PAD, NBLK), :] = part
        sa[pl.ds((2 * t + 1) * PAD, NBLK), :] = pltpu.roll(part, 64, 1)
    sp[0] = jnp.sqrt(prec[...].astype(F32))
    sp[1] = innov[...].astype(F32) * sp[0]

    def blocks(step, carry):
        for i in range(16):
            b = step * 16 + i
            x = sa[pl.ds(b, LEV, stride=PAD), :][:, :K].astype(BF16)
            y = lax.dot_general(x, w[b], (((0,), (0,)), ((), ())), preferred_element_type=F32)
            root = sp[0, pl.ds(b, 1), :]
            ys = (y * root).astype(BF16)
            forced = sp[1, pl.ds(b, 1), :]
            tail = jnp.where(lax.broadcasted_iota(jnp.int32, (16, 128), 0) == 0, forced, 0.0).astype(BF16)
            g = lax.dot_general(
                jnp.concatenate([ys, tail], 0), ys, (((1,), (1,)), ((), ())), preferred_element_type=F32
            )
            sg[pl.ds(b, 72, stride=PAD), 0:K] = g[:72]
        return carry

    lax.fori_loop(0, 2, blocks, 0)

    wide = lax.broadcasted_iota(jnp.int32, (NBLK, 128), 1)
    zeros64 = jnp.zeros((NBLK, K), F32)

    def unit(k):
        return sg[pl.ds(k * PAD, NBLK), 0:K]

    for j in range(32):
        gall[1, j] = jnp.concatenate([unit(j), unit(j + 32)], 1).astype(BF16)
    gall[1, 32] = jnp.concatenate([unit(64), zeros64], 1).astype(BF16)

    pl.semaphore_wait(barrier, 6)
    first = [
        remote(gall.at[1], gall.at[0], g_send.at[0], g_recv.at[0], (ia, east)),
        remote(gall.at[1], gall.at[2], g_send.at[1], g_recv.at[1], (ia, west)),
        remote(nbp.at[1], nbp.at[0], n_send.at[0], n_recv.at[0], (up, jb)),
        remote(nbp.at[1], nbp.at[2], n_send.at[1], n_recv.at[1], (down, jb)),
        remote(msend.at[0], mrecv.at[0], m_send.at[0], m_recv.at[0], (ia, east)),
        remote(msend.at[1], mrecv.at[1], m_send.at[1], m_recv.at[1], (ia, west)),
    ]
    for copy in (first[4], first[5], first[2], first[3], first[0], first[1]):
        copy.start()

    def columns_of(r, carry):
        x = jnp.concatenate([ens[r, :, 128 * t : 128 * (t + 1)] for t in range(16)], 0)
        spread = (x.astype(F32) - dot(x, averager)).astype(BF16).astype(F32)
        for t in range(16):
            sx[r, pl.ds(t * 17, CLON), :] = spread[CLON * t : CLON * (t + 1)]
        for c in range(CLON):
            xa[r * CLON + c] = sx[r, pl.ds(c, 16, stride=17), :].astype(BF16)
        return carry

    lax.fori_loop(0, CLAT, columns_of, 0)

    for copy in first[2:]:
        copy.wait()
    code3 = mrecv[0, 0:1, :] + code_own + mrecv[1, 0:1, :]
    is_live = (code3 > 0).astype(F32)
    place = jnp.maximum(code3 - 1, 0)
    b_row = (place // CLON).astype(F32)
    b_col = (place % CLON + (lane1 // NBLK - 1) * CLON).astype(F32)
    point = lax.broadcasted_iota(jnp.int32, (32, 128), 0)
    p_row = (2 * (point // 8)).astype(F32)
    p_col = (2 * (point % 8)).astype(F32)
    weights = []
    for u in (-1, 0, 1):
        listed = nbp[u + 1]
        count = jnp.zeros((32, 128), F32)
        for n in range(NNB):
            count += (listed[:, n : n + 1] - 96 * (u + 1) == wide).astype(F32)
        dlat = (b_row + float(u * CLAT)) - p_row
        dlon = b_col - p_col
        taper = jnp.exp(-(dlat * dlat + dlon * dlon) / (2.0 * LOC * LOC))
        valid = ((ia - u >= 0) & (ia - u < na)).astype(F32)
        weights.append(jnp.where(wide < 96, count * taper * is_live * valid, 0.0))
    whi, wlo = split(jnp.concatenate(weights, 0))
    lhs = jnp.concatenate([whi, wlo], 0)[:, :96]

    first[0].wait()
    first[1].wait()
    second = []
    for n, (lo, hi) in enumerate(CHUNKS):
        for t in range(lo, hi):
            rhs = jnp.concatenate([gall[0, t], gall[1, t], gall[2, t]], 0)
            o = dot(lhs, rhs)
            o = o[:96] + o[96:]
            ssend[0, t] = o[:32].astype(BF16)
            own[t] = o[32:64]
            ssend[1, t] = o[64:].astype(BF16)
        span = pl.ds(lo, hi - lo)
        pair = [
            remote(ssend.at[0, span], srecv.at[0, span], s_send.at[0, n], s_recv.at[0, n], (down, jb)),
            remote(ssend.at[1, span], srecv.at[1, span], s_send.at[1, n], s_recv.at[1, n], (up, jb)),
        ]
        for copy in pair:
            copy.start()
        second.append(pair)
    for n, (lo, hi) in enumerate(CHUNKS):
        for copy in second[n]:
            copy.wait()
        for t in range(lo, hi):
            s2[pl.ds(t * PAD, 32), :] = own[t] + srecv[0, t].astype(F32) + srecv[1, t].astype(F32)

    row64 = lax.broadcasted_iota(jnp.int32, (K, 256), 0)
    lane256 = lax.broadcasted_iota(jnp.int32, (K, 256), 1)
    eye = (lane256 % 64 == row64).astype(F32)
    ones = jnp.where(
        lax.broadcasted_iota(jnp.int32, (256, 256), 0) // 64 == lax.broadcasted_iota(jnp.int32, (256, 256), 1) // 64,
        1.0, 0.0,
    ).astype(BF16)
    half = lax.broadcasted_iota(jnp.int32, (32, 128), 1) < 64
    half1 = lane1 < 64
    row16 = lax.broadcasted_iota(jnp.int32, (16, 256), 0)

    def two_rows(x):
        hi = x.astype(BF16).astype(F32)
        return jnp.where(row16 == 0, hi, jnp.where(row16 == 1, x - hi, 0.0)).astype(BF16)

    def product(a_hi, a_lo, b):
        b_hi, b_lo = split(b)
        o = dot(jnp.concatenate([a_hi, a_lo], 0), diagonal(b_hi, left, right))
        return o[:K] + o[K:] + dot(a_hi, diagonal(b_lo, left, right))

    def keep(g, y, z):
        y_hi, y_lo = split(y)
        z_hi, z_lo = split(z)
        yz[g, 0:64] = y_hi
        yz[g, 64:128] = z_hi
        yz[g, 128:192] = y_lo
        yz[g, 192:256] = z_lo

    for g in range(8):
        parts, proj = [], []
        for m in (2 * g, 2 * g + 1):
            x0 = s2[pl.ds(2 * m, 32, stride=PAD), :]
            x1 = s2[pl.ds(2 * m + 1, 32, stride=PAD), :]
            parts.append(
                jnp.concatenate(
                    [jnp.where(half, x0, pltpu.roll(x1, 64, 1)), jnp.where(half, pltpu.roll(x0, 64, 1), x1)], 0
                )
            )
            q0 = s2[pl.ds(32 * PAD + 2 * m, 1), :]
            q1 = s2[pl.ds(32 * PAD + 2 * m + 1, 1), :]
            proj.append(jnp.where(half1, q0, pltpu.roll(q1, 64, 1)))
        gram = jnp.concatenate(parts, 1) + (K - 1.0) * eye
        sums = dot(two_rows(jnp.sum(gram * gram, axis=0, keepdims=True)), ones)
        inv = 1.0 / jnp.sqrt(sums[0:1] + sums[1:2])
        scales[g, 0:1] = inv
        scales[g, 1:2] = jnp.concatenate(proj, 1)
        x = gram * inv
        middle = 1.5 * eye - 0.5 * x
        x_hi, x_lo = split(x)
        keep(g, product(x_hi, x_lo, middle), middle)

    def middle_of(g):
        z_hi, z_lo = yz[g, 64:128], yz[g, 192:256]
        o = dot(jnp.concatenate([z_hi, z_lo], 0), diagonal(yz[g, 0:64], left, right))
        o = o[:K] + o[K:] + dot(z_hi, diagonal(yz[g, 128:192], left, right))
        return 1.5 * eye - 0.5 * o

    def turn(step, carry):
        for g in range(8):
            zf[g] = middle_of(g)
        for g in range(8):
            m_hi, m_lo = split(zf[g])
            o = dot(yz[g], diagonal(m_hi, left, right))
            e = dot(yz[g, 0:128], diagonal(m_lo, left, right))
            keep(g, o[0:64] + o[128:192] + e[0:64], o[64:128] + o[192:256] + e[64:128])
        return carry

    lax.fori_loop(0, NSI - 2, turn, 0)
    for g in range(8):
        zf[g] = product(yz[g, 64:128], yz[g, 192:256], middle_of(g))
    for g in range(8):
        z = zf[g]
        z_hi, z_lo = split(z)
        inv = scales[g, 0:1]
        o = dot(two_rows(scales[g, 1:2]), diagonal(z_hi, left, right))
        e = dot(two_rows(scales[g, 1:2]), diagonal(z_lo, left, right))
        h = o[0:1] + o[1:2] + e[0:1]
        d_hi, d_lo = split(z * h)
        s = dot(jnp.concatenate([d_hi, d_lo], 0), ones)
        t = z * (jnp.sqrt(K - 1.0) * jnp.sqrt(inv)) + (s[:K] + s[K:]) * inv
        tb[2 * g] = t[:, :128].astype(BF16)
        tb[2 * g + 1] = t[:, 128:].astype(BF16)

    half64 = lax.broadcasted_iota(jnp.int32, (K, 128), 1) < 64
    for i in range(2):
        p0 = tb[8 * i].astype(F32)
        p1 = tb[8 * i + 4].astype(F32)
        csend[i] = jnp.where(half64, p0, pltpu.roll(p1, 64, 1)).astype(BF16)
    third = [
        remote(tb.at[pl.ds(0, 4)], rrow, t_send.at[0], t_recv.at[0], (up, jb)),
        remote(csend, rcol, t_send.at[1], t_recv.at[1], (ia, west)),
        remote(csend.at[0], rcor, t_send.at[2], t_recv.at[2], (up, west)),
    ]
    for copy in third:
        copy.start()

    zero64 = jnp.zeros((K, 128), F32)

    def expand(pair):
        v = pair.astype(F32)
        r = pltpu.roll(v, 64, 1)
        d0 = jnp.concatenate([jnp.where(half64, v, zero64), jnp.where(half64, zero64, r)], 0)
        d1 = jnp.concatenate([jnp.where(half64, r, zero64), jnp.where(half64, zero64, v)], 0)
        return d0.astype(BF16), d1.astype(BF16)

    for m in range(16):
        a, c = m // 4, 2 * (m % 4)
        dd[a, c], dd[a, c + 1] = expand(tb[m])

    last = ia == na - 1
    for copy in third:
        copy.wait()
    edge = last.astype(F32)
    for i in range(4):
        mixed = rrow[i].astype(F32) * (1.0 - edge) + tb[12 + i].astype(F32) * edge
        dd[4, 2 * i], dd[4, 2 * i + 1] = expand(mixed)
    for i in range(2):
        dd[2 * i, 8], dd[2 * i + 1, 8] = expand(rcol[i])
    bottom = pltpu.roll(rcol[1].astype(F32), 64, 1)
    dd[4, 8] = expand(rcor[...].astype(F32) * (1.0 - edge) + bottom * edge)[0]

    def finish(a, carry):
        none = jnp.zeros((16, 128), BF16)
        for c in range(8):
            base = 2 * a * CLON + 2 * c
            ee, eo = xa[base], xa[base + 1] * 0.5
            oe, oo = xa[base + CLON] * 0.5, xa[base + CLON + 1] * 0.25
            lower = jnp.concatenate([jnp.concatenate([oe, none], 1), jnp.concatenate([oo, oo], 1)], 0)
            upper = jnp.concatenate([jnp.concatenate([ee, none], 1), jnp.concatenate([eo, eo], 1), lower], 0)
            o = dot(upper, dd[a, c : c + 2].reshape(256, 128))
            e = dot(lower, dd[a + 1, c : c + 2].reshape(256, 128))
            so[0, pl.ds(2 * c, 16, stride=17), :] = o[0:16]
            so[0, pl.ds(2 * c + 1, 16, stride=17), :] = o[16:32]
            so[1, pl.ds(2 * c, 16, stride=17), :] = o[32:48] + e[0:16]
            so[1, pl.ds(2 * c + 1, 16, stride=17), :] = o[48:64] + e[16:32]
        for i in range(2):
            r = 2 * a + i
            x = jnp.concatenate([ens[r, :, 128 * t : 128 * (t + 1)] for t in range(16)], 0)
            center = dot(x, averager)
            for t in range(16):
                rows = so[i, pl.ds(t * 17, CLON), :] + center[CLON * t : CLON * (t + 1)]
                out[r, :, 128 * t : 128 * (t + 1)] = rows.astype(BF16)
        return carry

    lax.fori_loop(0, 4, finish, 0)


def solution(mesh):
    na, nb = mesh.shape["lat"], mesh.shape["lon"]

    def body(ensemble, channel_weights, block_column, innovation, error_precision, block_count, neighbours):
        vmem = pl.BlockSpec(memory_space=pltpu.VMEM)
        smem = pl.BlockSpec(memory_space=pltpu.SMEM)
        dma = pltpu.SemaphoreType.DMA
        return pl.pallas_call(
            functools.partial(kernel, na, nb),
            out_shape=jax.ShapeDtypeStruct(ensemble.shape, BF16),
            in_specs=[vmem, vmem, vmem, vmem, vmem, smem, vmem],
            out_specs=vmem,
            scratch_shapes=[
                pltpu.VMEM((LEV * PAD, 128), F32),
                pltpu.VMEM((72 * PAD, 128), F32),
                pltpu.VMEM((2, NBLK, OB), F32),
                pltpu.VMEM((3, NT, NBLK, 128), BF16),
                pltpu.VMEM((3, 32, 128), jnp.int32),
                pltpu.VMEM((2, 8, 128), jnp.int32),
                pltpu.VMEM((2, 8, 128), jnp.int32),
                pltpu.VMEM((2, NT, 32, 128), BF16),
                pltpu.VMEM((2, NT, 32, 128), BF16),
                pltpu.VMEM((NT, 32, 128), F32),
                pltpu.VMEM((NT * PAD, 128), F32),
                pltpu.VMEM((8, 256, 256), BF16),
                pltpu.VMEM((8, K, 256), F32),
                pltpu.VMEM((16, K, 128), BF16),
                pltpu.VMEM((2, K, 128), BF16),
                pltpu.VMEM((4, K, 128), BF16),
                pltpu.VMEM((2, K, 128), BF16),
                pltpu.VMEM((K, 128), BF16),
                pltpu.VMEM((5, 9, 128, 128), BF16),
                pltpu.VMEM((CLAT * CLON, 16, 128), BF16),
                pltpu.VMEM((CLAT, 272, 128), F32),
                pltpu.VMEM((2, 272, 128), F32),
                pltpu.VMEM((8, 8, 256), F32),
                dma((2,)), dma((2,)), dma((2,)), dma((2,)), dma((2,)), dma((2,)),
                dma((2, 3)), dma((2, 3)), dma((3,)), dma((3,)),
            ],
            compiler_params=pltpu.CompilerParams(
                collective_id=0, has_side_effects=True, vmem_limit_bytes=48 * 2**20
            ),
        )(
            ensemble,
            channel_weights[0, 0],
            block_column[0],
            innovation[0, 0],
            error_precision[0, 0],
            block_count,
            neighbours.reshape(32, NNB),
        )

    return jax.shard_map(
        body,
        mesh=mesh,
        in_specs=(
            P("lat", "lon", None),
            P("lat", "lon", None, None, None),
            P("lat", "lon", None),
            P("lat", "lon", None, None),
            P("lat", "lon", None, None),
            P("lat", "lon"),
            P("lat", "lon", None),
        ),
        out_specs=P("lat", "lon", None),
        check_vma=False,
    )
```

```python
import functools

import jax
import jax.numpy as jnp
from jax import lax
from jax.experimental import pallas as pl
from jax.experimental.pallas import tpu as pltpu
from jax.sharding import PartitionSpec as P

F32 = jnp.float32
BF16 = jnp.bfloat16
MESH = pl.DeviceIdType.MESH
NSI = 6
LOC = 12
K = 64
OB = 128
CLAT = 8
CLON = 16
NBLK = 32
NNB = 12
LEV = 32
NT = 17
PAD = 33
CHUNKS = ((0, 4), (4, 8), (8, 12), (12, 17))
ORDER = (0, 1, 2, 3, 4, 5, 6, 7, 8, 16, 24, 9, 10, 11, 12, 13, 14, 15) + tuple(range(17, 24)) + tuple(range(25, 32))


def dot(a, b):
    return jnp.dot(a, b, preferred_element_type=F32)


def split(x):
    hi = x.astype(BF16)
    return hi, (x - hi.astype(F32)).astype(BF16)


def diagonal(x, left, right):
    first, second = x[:, :128], x[:, 128:]
    zero = jnp.zeros_like(first)
    return jnp.concatenate(
        [
            jnp.concatenate([first * left, zero], 1),
            jnp.concatenate([first * right, zero], 1),
            jnp.concatenate([zero, second * left], 1),
            jnp.concatenate([zero, second * right], 1),
        ],
        0,
    )


def kernel(
    na, nb, ens_h, w_h, bcol_h, innov_h, prec_h, cnt_h, nbs_h, out,
    ens, w, bcol, innov, prec, cnt, nbs, in_sem, yb, sa, sg, sp, gall, nbp, msend, mrecv, ssend, srecv, own, s2, yz, zf, tb, csend, rrow, rcol, rcor, dd, xa, sx, so,
    scales, g_send, g_recv, n_send, n_recv, m_send, m_recv, s_send, s_recv, t_send, t_recv,
):
    loads = [
        pltpu.make_async_copy(src, dst, in_sem.at[i])
        for i, (src, dst) in enumerate(
            ((bcol_h, bcol), (cnt_h, cnt), (ens_h, ens), (w_h, w), (prec_h, prec), (innov_h, innov), (nbs_h, nbs))
        )
    ]
    for load in loads:
        load.start()
    ia, jb = lax.axis_index("lat"), lax.axis_index("lon")
    up, down = lax.rem(ia + na - 1, na), lax.rem(ia + 1, na)
    west, east = lax.rem(jb + nb - 1, nb), lax.rem(jb + 1, nb)

    barrier = pltpu.get_barrier_semaphore()
    for peer in ((up, jb), (down, jb), (ia, west), (ia, east), (up, west), (down, east)):
        pl.semaphore_signal(barrier, inc=1, device_id=peer, device_id_type=MESH)

    def remote(src, dst, send, recv, peer):
        return pltpu.make_async_remote_copy(
            src_ref=src, dst_ref=dst, send_sem=send, recv_sem=recv, device_id=peer, device_id_type=MESH
        )

    lane1 = lax.broadcasted_iota(jnp.int32, (1, 128), 1)
    left_f = (lane1 < 64).astype(F32)
    left, right = left_f.astype(BF16), (1.0 - left_f).astype(BF16)
    row128 = lax.broadcasted_iota(jnp.int32, (128, 128), 0)
    lane128 = lax.broadcasted_iota(jnp.int32, (128, 128), 1)
    averager = jnp.where(row128 // 64 == lane128 // 64, 1.0 / K, 0.0).astype(BF16)

    for load in loads:
        load.wait()

    code = jnp.zeros((1, 128), jnp.int32)
    columns = jnp.concatenate([bcol[...], jnp.zeros((1, 128 - NBLK), jnp.int32)], 1)
    live = (lane1 < cnt[0, 0]) & (lane1 < NBLK)
    code = jnp.where(live, columns + 1, 0)
    msend[0] = jnp.broadcast_to(code, (8, 128))
    msend[1] = jnp.broadcast_to(pltpu.roll(code, 2 * NBLK, 1), (8, 128))
    code_own = pltpu.roll(code, NBLK, 1)
    for to, start, rows in ((0, 0, 8), (8, 8, 1), (9, 16, 1), (10, 24, 1), (11, 9, 7), (18, 17, 7), (25, 25, 7)):
        nbp[1, to : to + rows, 0:NNB] = nbs[start : start + rows]

    chosen = jnp.where(row128 == jnp.broadcast_to(columns, (128, 128)), 1.0, 0.0)
    chosen = jnp.where(lane128 < NBLK, chosen, 0.0)
    chosen = jnp.transpose(chosen)[:NBLK].astype(BF16)
    state = ens[...].reshape(CLAT * CLON, LEV * K)
    picked = dot(chosen, state)
    stacked = jnp.concatenate([picked[:, 128 * t : 128 * (t + 1)] for t in range(16)], 0)
    anomaly = stacked - dot(stacked.astype(BF16), averager)
    for t in range(16):
        part = anomaly[NBLK * t : NBLK * (t + 1)]
        sa[pl.ds(2 * t * PAD, NBLK), :] = part
        sa[pl.ds((2 * t + 1) * PAD, NBLK), :] = pltpu.roll(part, 64, 1)
    sp[0] = jnp.sqrt(prec[...].astype(F32))
    sp[1] = innov[...].astype(F32) * sp[0]

    U1, U2, REP = 32, 32, 1

    def observed(step, carry):
        for i in range(U1):
            b = lax.rem(step, 32 // U1) * U1 + i
            x = sa[pl.ds(b, LEV, stride=PAD), :][:, :K].astype(BF16)
            y = lax.dot_general(x, w[b], (((0,), (0,)), ((), ())), preferred_element_type=F32)
            yb[b, 0:K] = (y * sp[0, pl.ds(b, 1), :]).astype(BF16)
            forced = sp[1, pl.ds(b, 1), :]
            yb[b, K : K + 16] = jnp.where(lax.broadcasted_iota(jnp.int32, (16, 128), 0) == 0, forced, 0.0).astype(BF16)
        return carry

    def squared(step, carry):
        for i in range(U2):
            b = lax.rem(step, 32 // U2) * U2 + i
            g = lax.dot_general(yb[b], yb[b, 0:K], (((1,), (1,)), ((), ())), preferred_element_type=F32)
            sg[pl.ds(b, 72, stride=PAD), 0:K] = g[:72]
        return carry

    lax.fori_loop(0, 32 // U1 * REP, observed, 0)
    lax.fori_loop(0, 32 // U2 * REP, squared, 0)

    wide = lax.broadcasted_iota(jnp.int32, (NBLK, 128), 1)
    def unit(k):
        return sg[pl.ds(k * PAD, NBLK), :]

    for i in range(16):
        k = i + 16
        low = unit(i) if i == 0 else jnp.where(wide >= i, unit(i), pltpu.roll(unit(63 - i), 64 + i, 1))
        high = jnp.where(wide >= 64 + k, pltpu.roll(unit(k), 64, 1), pltpu.roll(unit(63 - k), k, 1))
        gall[1, i] = jnp.where(wide < 64, low, high).astype(BF16)
    spine = jnp.zeros((NBLK, 128), F32)
    for k in range(32, 64):
        spine = jnp.where(wide == k, unit(k), spine)
    gall[1, 16] = jnp.where(wide < 64, unit(64), pltpu.roll(spine, 64, 1)).astype(BF16)

    pl.semaphore_wait(barrier, 6)
    facts = [
        remote(nbp.at[1], nbp.at[0], n_send.at[0], n_recv.at[0], (up, jb)),
        remote(nbp.at[1], nbp.at[2], n_send.at[1], n_recv.at[1], (down, jb)),
        remote(msend.at[0], mrecv.at[0], m_send.at[0], m_recv.at[0], (ia, east)),
        remote(msend.at[1], mrecv.at[1], m_send.at[1], m_recv.at[1], (ia, west)),
    ]
    first = []
    for n, (lo, hi) in enumerate(CHUNKS):
        span = pl.ds(lo, hi - lo)
        first.append(
            [
                remote(gall.at[1, span], gall.at[0, span], g_send.at[0, n], g_recv.at[0, n], (ia, east)),
                remote(gall.at[1, span], gall.at[2, span], g_send.at[1, n], g_recv.at[1, n], (ia, west)),
            ]
        )
    for copy in facts + [copy for pair in first for copy in pair]:
        copy.start()

    def columns_of(r, carry):
        x = jnp.concatenate([ens[r, :, 128 * t : 128 * (t + 1)] for t in range(16)], 0)
        spread = (x.astype(F32) - dot(x, averager)).astype(BF16).astype(F32)
        for t in range(16):
            sx[r, pl.ds(t * 17, CLON), :] = spread[CLON * t : CLON * (t + 1)]
        for c in range(CLON):
            xa[r * CLON + c] = sx[r, pl.ds(c, 16, stride=17), :].astype(BF16)
        return carry

    lax.fori_loop(0, CLAT, columns_of, 0)

    for copy in facts:
        copy.wait()
    code3 = mrecv[0, 0:1, :] + code_own + mrecv[1, 0:1, :]
    is_live = (code3 > 0).astype(F32)
    place = jnp.maximum(code3 - 1, 0)
    b_row = (place // CLON).astype(F32)
    b_col = (place % CLON + (lane1 // NBLK - 1) * CLON).astype(F32)
    point = lax.broadcasted_iota(jnp.int32, (32, 128), 0)
    point = jnp.where(
        point < 8,
        point,
        jnp.where(point < 11, 8 * (point - 7), jnp.where(point < 18, point - 2, jnp.where(point < 25, point - 1, point))),
    )
    p_row = (2 * (point // 8)).astype(F32)
    p_col = (2 * (point % 8)).astype(F32)
    weights = []
    for u in (-1, 0, 1):
        listed = nbp[u + 1]
        count = jnp.zeros((32, 128), F32)
        for n in range(NNB):
            count += (listed[:, n : n + 1] - 96 * (u + 1) == wide).astype(F32)
        dlat = (b_row + float(u * CLAT)) - p_row
        dlon = b_col - p_col
        taper = jnp.exp(-(dlat * dlat + dlon * dlon) / (2.0 * LOC * LOC))
        valid = ((ia - u >= 0) & (ia - u < na)).astype(F32)
        weights.append(jnp.where(wide < 96, count * taper * is_live * valid, 0.0))
    whi, wlo = split(jnp.concatenate(weights, 0))
    lhs = jnp.concatenate([whi, wlo], 0)[:, :96]

    second = []
    for n, (lo, hi) in enumerate(CHUNKS):
        for copy in first[n]:
            copy.wait()
        for t in range(lo, hi, 2):
            ts = range(t, min(t + 2, hi))
            rhs = jnp.concatenate([jnp.concatenate([gall[v, i] for i in ts], 1) for v in range(3)], 0)
            o = dot(lhs, rhs)
            o = o[:96] + o[96:]
            for i in ts:
                part = o[:, 128 * (i - t) : 128 * (i - t + 1)]
                ssend[0, i] = part[:32].astype(BF16)
                own[i] = part[32:64]
                ssend[1, i] = part[64:].astype(BF16)
        span = pl.ds(lo, hi - lo)
        pair = [
            remote(ssend.at[0, span], srecv.at[0, span], s_send.at[0, n], s_recv.at[0, n], (down, jb)),
            remote(ssend.at[1, span], srecv.at[1, span], s_send.at[1, n], s_recv.at[1, n], (up, jb)),
        ]
        for copy in pair:
            copy.start()
        second.append(pair)
    for n, (lo, hi) in enumerate(CHUNKS):
        for copy in second[n]:
            copy.wait()
        for i in range(lo, hi):
            tile = own[i] + srecv[0, i].astype(F32) + srecv[1, i].astype(F32)
            if i == 16:
                s2[pl.ds(64 * PAD, 32), :] = tile
                s2[pl.ds(65 * PAD, 32), :] = pltpu.roll(tile, 64, 1)
                continue
            k = i + 16
            s2[pl.ds(i * PAD, 32), :] = tile
            s2[pl.ds((63 - i) * PAD, 32), :] = pltpu.roll(tile, 64 - i, 1)
            s2[pl.ds(k * PAD, 32), :] = pltpu.roll(tile, 64, 1)
            s2[pl.ds((63 - k) * PAD, 32), :] = pltpu.roll(tile, 128 - k, 1)
    row64 = lax.broadcasted_iota(jnp.int32, (K, 256), 0)
    lane256 = lax.broadcasted_iota(jnp.int32, (K, 256), 1)
    eye = (lane256 % 64 == row64).astype(F32)
    ones = jnp.where(
        lax.broadcasted_iota(jnp.int32, (256, 256), 0) // 64 == lax.broadcasted_iota(jnp.int32, (256, 256), 1) // 64,
        1.0, 0.0,
    ).astype(BF16)
    half64 = lax.broadcasted_iota(jnp.int32, (K, 128), 1) < 64
    row_k = lax.broadcasted_iota(jnp.int32, (K, 128), 0)
    lane_k = lax.broadcasted_iota(jnp.int32, (K, 128), 1)
    above = (lane_k > row_k) & (lane_k < 64)
    first_diagonal = (lane_k == row_k) & (row_k < 32)
    last_diagonal = (lane_k == row_k) & (row_k >= 32)
    half1 = lane1 < 64
    row16 = lax.broadcasted_iota(jnp.int32, (16, 256), 0)

    def two_rows(x):
        hi = x.astype(BF16).astype(F32)
        return jnp.where(row16 == 0, hi, jnp.where(row16 == 1, x - hi, 0.0)).astype(BF16)

    def product(a_hi, a_lo, b):
        b_hi, b_lo = split(b)
        o = dot(jnp.concatenate([a_hi, a_lo], 0), diagonal(b_hi, left, right))
        return o[:K] + o[K:] + dot(a_hi, diagonal(b_lo, left, right))

    def keep(g, y, z):
        y_hi, y_lo = split(y)
        z_hi, z_lo = split(z)
        yz[g, 0:64] = y_hi
        yz[g, 64:128] = z_hi
        yz[g, 128:192] = y_lo
        yz[g, 192:256] = z_lo

    def symmetric(m):
        upper, own_diagonal = [], []
        for p in (2 * m, 2 * m + 1):
            v = s2[pl.ds(p, K, stride=PAD), :]
            d = jnp.broadcast_to(s2[pl.ds(65 * PAD + p, 1), :], (K, 128))
            upper.append(jnp.where(above, v, 0.0))
            own_diagonal.append(jnp.where(first_diagonal, v, jnp.where(last_diagonal, d, 0.0)))
        whole = jnp.transpose(jnp.concatenate(upper, 0))[:K]
        second_half = pltpu.roll(upper[1] + own_diagonal[1], 64, 1)
        return whole + jnp.where(half64, upper[0] + own_diagonal[0], second_half)

    def begin(g):
        parts, proj = [], []
        for m in (2 * g, 2 * g + 1):
            parts.append(symmetric(m))
            q0 = s2[pl.ds(64 * PAD + 2 * m, 1), :]
            q1 = s2[pl.ds(64 * PAD + 2 * m + 1, 1), :]
            proj.append(jnp.where(half1, q0, pltpu.roll(q1, 64, 1)))
        gram = jnp.concatenate(parts, 1) + (K - 1.0) * eye
        zf[g] = gram
        scales[g, 1:2] = jnp.concatenate(proj, 1)
        scales[g, 0:1] = jnp.sum(gram * gram, axis=0, keepdims=True)

    def scale(g):
        sums = dot(two_rows(scales[g, 0:1]), ones)
        scales[g, 0:1] = 1.0 / jnp.sqrt(sums[0:1] + sums[1:2])

    def first_step(g):
        x = zf[g] * scales[g, 0:1]
        middle = 1.5 * eye - 0.5 * x
        x_hi, x_lo = split(x)
        keep(g, product(x_hi, x_lo, middle), middle)

    def middle_of(g):
        z_hi, z_lo = yz[g, 64:128], yz[g, 192:256]
        o = dot(jnp.concatenate([z_hi, z_lo], 0), diagonal(yz[g, 0:64], left, right))
        o = o[:K] + o[K:] + dot(z_hi, diagonal(yz[g, 128:192], left, right))
        return 1.5 * eye - 0.5 * o

    SEP = 1
    def apart(f):
        if SEP:
            pl.when(ia >= 0)(f)
        else:
            f()

    def invert(groups):
        def opening():
            for g in groups:
                begin(g)
        apart(opening)
        def scaling():
            for g in groups:
                scale(g)
        apart(scaling)
        def start():
            for g in groups:
                first_step(g)
        apart(start)

        def turn(step, carry):
            def one():
                for g in groups:
                    zf[g] = middle_of(g)
            apart(one)
            def two():
                for g in groups:
                    m_hi, m_lo = split(zf[g])
                    o = dot(yz[g], diagonal(m_hi, left, right))
                    e = dot(yz[g, 0:128], diagonal(m_lo, left, right))
                    keep(g, o[0:64] + o[128:192] + e[0:64], o[64:128] + o[192:256] + e[64:128])
            apart(two)
            return carry

        lax.fori_loop(0, NSI - 2, turn, 0)
        def three():
            for g in groups:
                zf[g] = middle_of(g)
        apart(three)
        def four():
            for g in groups:
                zf[g] = product(yz[g, 64:128], yz[g, 192:256], zf[g])
        apart(four)
        def five():
            for g in groups:
                z_hi, z_lo = split(zf[g])
                o = dot(two_rows(scales[g, 1:2]), diagonal(z_hi, left, right))
                e = dot(two_rows(scales[g, 1:2]), diagonal(z_lo, left, right))
                scales[g, 2:3] = o[0:1] + o[1:2] + e[0:1]
        apart(five)
        def six():
            for g in groups:
                z = zf[g]
                inv = scales[g, 0:1]
                d_hi, d_lo = split(z * scales[g, 2:3])
                s = dot(jnp.concatenate([d_hi, d_lo], 0), ones)
                t = z * (jnp.sqrt(K - 1.0) * jnp.sqrt(inv)) + (s[:K] + s[K:]) * inv
                tb[2 * g] = t[:, :128].astype(BF16)
                tb[2 * g + 1] = t[:, 128:].astype(BF16)
        apart(six)

    split_ns = 1
    invert(range(4) if split_ns else range(8))

    p0, p8, p10 = tb[0].astype(F32), tb[4].astype(F32), tb[5].astype(F32)
    csend[0] = jnp.where(half64, p0, pltpu.roll(p8, 64, 1)).astype(BF16)
    csend[1] = jnp.where(half64, pltpu.roll(p8, 64, 1), pltpu.roll(p10, 64, 1)).astype(BF16)
    third = [
        remote(tb.at[pl.ds(0, 4)], rrow, t_send.at[0], t_recv.at[0], (up, jb)),
        remote(csend, rcol, t_send.at[1], t_recv.at[1], (ia, west)),
        remote(csend.at[0], rcor, t_send.at[2], t_recv.at[2], (up, west)),
    ]
    for copy in third:
        copy.start()
    if split_ns:
        invert(range(4, 8))
    zero64 = jnp.zeros((K, 128), F32)

    def expand(pair):
        v = pair.astype(F32)
        r = pltpu.roll(v, 64, 1)
        d0 = jnp.concatenate([jnp.where(half64, v, zero64), jnp.where(half64, zero64, r)], 0)
        d1 = jnp.concatenate([jnp.where(half64, r, zero64), jnp.where(half64, zero64, v)], 0)
        return d0.astype(BF16), d1.astype(BF16)

    for m in range(16):
        for p, d in zip(ORDER[2 * m : 2 * m + 2], expand(tb[m])):
            dd[p // 8, p % 8] = d

    last = ia == na - 1
    for copy in third:
        copy.wait()
    edge = last.astype(F32)
    for i in range(4):
        for c, d in zip((2 * i, 2 * i + 1), expand(rrow[i])):
            dd[4, c] = (d.astype(F32) * (1.0 - edge) + dd[3, c].astype(F32) * edge).astype(BF16)
    for i in range(2):
        dd[2 * i, 8], dd[2 * i + 1, 8] = expand(rcol[i])
    bottom = pltpu.roll(rcol[1].astype(F32), 64, 1)
    dd[4, 8] = expand(rcor[...].astype(F32) * (1.0 - edge) + bottom * edge)[0]

    def finish(a, carry):
        none = jnp.zeros((16, 128), BF16)
        for c in range(8):
            base = 2 * a * CLON + 2 * c
            ee, eo = xa[base], xa[base + 1] * 0.5
            oe, oo = xa[base + CLON] * 0.5, xa[base + CLON + 1] * 0.25
            lower = jnp.concatenate([jnp.concatenate([oe, none], 1), jnp.concatenate([oo, oo], 1)], 0)
            upper = jnp.concatenate([jnp.concatenate([ee, none], 1), jnp.concatenate([eo, eo], 1), lower], 0)
            o = dot(upper, dd[a, c : c + 2].reshape(256, 128))
            e = dot(lower, dd[a + 1, c : c + 2].reshape(256, 128))
            so[0, pl.ds(2 * c, 16, stride=17), :] = o[0:16]
            so[0, pl.ds(2 * c + 1, 16, stride=17), :] = o[16:32]
            so[1, pl.ds(2 * c, 16, stride=17), :] = o[32:48] + e[0:16]
            so[1, pl.ds(2 * c + 1, 16, stride=17), :] = o[48:64] + e[16:32]
        for i in range(2):
            r = 2 * a + i
            x = jnp.concatenate([ens[r, :, 128 * t : 128 * (t + 1)] for t in range(16)], 0)
            center = dot(x, averager)
            for t in range(16):
                rows = so[i, pl.ds(t * 17, CLON), :] + center[CLON * t : CLON * (t + 1)]
                out[r, :, 128 * t : 128 * (t + 1)] = rows.astype(BF16)
        return carry

    lax.fori_loop(0, 4, finish, 0)


def solution(mesh):
    na, nb = mesh.shape["lat"], mesh.shape["lon"]

    def body(ensemble, channel_weights, block_column, innovation, error_precision, block_count, neighbours):
        vmem = pl.BlockSpec(memory_space=pltpu.VMEM)
        dma = pltpu.SemaphoreType.DMA
        return pl.pallas_call(
            functools.partial(kernel, na, nb),
            out_shape=jax.ShapeDtypeStruct(ensemble.shape, BF16),
            in_specs=[pl.BlockSpec(memory_space=pl.ANY)] * 7,
            out_specs=vmem,
            scratch_shapes=[
                pltpu.VMEM(ensemble.shape, BF16),
                pltpu.VMEM((NBLK, LEV, OB), BF16),
                pltpu.VMEM((1, NBLK), jnp.int32),
                pltpu.VMEM((NBLK, OB), BF16),
                pltpu.VMEM((NBLK, OB), BF16),
                pltpu.SMEM((1, 1), jnp.int32),
                pltpu.VMEM((32, NNB), jnp.int32),
                dma((7,)),
                pltpu.VMEM((NBLK, K + 16, OB), BF16),
                pltpu.VMEM((LEV * PAD, 128), F32),
                pltpu.VMEM((72 * PAD, 128), F32),
                pltpu.VMEM((2, NBLK, OB), F32),
                pltpu.VMEM((3, NT, NBLK, 128), BF16),
                pltpu.VMEM((3, 32, 128), jnp.int32),
                pltpu.VMEM((2, 8, 128), jnp.int32),
                pltpu.VMEM((2, 8, 128), jnp.int32),
                pltpu.VMEM((2, NT, 32, 128), BF16),
                pltpu.VMEM((2, NT, 32, 128), BF16),
                pltpu.VMEM((NT, 32, 128), F32),
                pltpu.VMEM((66 * PAD, 128), F32),
                pltpu.VMEM((8, 256, 256), BF16),
                pltpu.VMEM((8, K, 256), F32),
                pltpu.VMEM((16, K, 128), BF16),
                pltpu.VMEM((2, K, 128), BF16),
                pltpu.VMEM((4, K, 128), BF16),
                pltpu.VMEM((2, K, 128), BF16),
                pltpu.VMEM((K, 128), BF16),
                pltpu.VMEM((5, 9, 128, 128), BF16),
                pltpu.VMEM((CLAT * CLON, 16, 128), BF16),
                pltpu.VMEM((CLAT, 272, 128), F32),
                pltpu.VMEM((2, 272, 128), F32),
                pltpu.VMEM((8, 8, 256), F32),
                dma((2, 4)), dma((2, 4)), dma((2,)), dma((2,)), dma((2,)), dma((2,)),
                dma((2, 4)), dma((2, 4)), dma((3,)), dma((3,)),
            ],
            compiler_params=pltpu.CompilerParams(
                collective_id=0, has_side_effects=True, vmem_limit_bytes=60 * 2**20
            ),
        )(
            ensemble,
            channel_weights[0, 0],
            block_column[0],
            innovation[0, 0],
            error_precision[0, 0],
            block_count,
            neighbours.reshape(32, NNB),
        )

    return jax.shard_map(
        body,
        mesh=mesh,
        in_specs=(
            P("lat", "lon", None),
            P("lat", "lon", None, None, None),
            P("lat", "lon", None),
            P("lat", "lon", None, None),
            P("lat", "lon", None, None),
            P("lat", "lon"),
            P("lat", "lon", None),
        ),
        out_specs=P("lat", "lon", None),
        check_vma=False,
    )
```

```python
import functools

import jax
import jax.numpy as jnp
from jax import lax
from jax.experimental import pallas as pl
from jax.experimental.pallas import tpu as pltpu
from jax.sharding import PartitionSpec as P

F32 = jnp.float32
BF16 = jnp.bfloat16
MESH = pl.DeviceIdType.MESH
NSI = 6
LOC = 12
K = 64
OB = 128
CLAT = 8
CLON = 16
NBLK = 32
NNB = 12
LEV = 32
NT = 17
PAD = 33
CHUNKS = ((0, 4), (4, 8), (8, 12), (12, 17))
ORDER = (0, 1, 2, 3, 4, 5, 6, 7, 8, 16, 24, 9, 10, 11, 12, 13, 14, 15) + tuple(range(17, 24)) + tuple(range(25, 32))


def dot(a, b):
    return jnp.dot(a, b, preferred_element_type=F32)


def split(x):
    hi = x.astype(BF16)
    return hi, (x - hi.astype(F32)).astype(BF16)


def diagonal(x, left, right):
    first, second = x[:, :128], x[:, 128:]
    zero = jnp.zeros_like(first)
    return jnp.concatenate(
        [
            jnp.concatenate([first * left, zero], 1),
            jnp.concatenate([first * right, zero], 1),
            jnp.concatenate([zero, second * left], 1),
            jnp.concatenate([zero, second * right], 1),
        ],
        0,
    )


def kernel(
    na, nb, ens_h, w_h, bcol_h, innov_h, prec_h, cnt, nbs_h, out,
    out_v, o_sem, pf, yf, ens, w, bcol, innov, prec, nbs, in_sem, yb, sa, sg, sp, gall, nbp, msend, mrecv, ssend, srecv, own, s2, zf, tb, csend, rrow, rcol, rcor, dd, xa, sx, so,
    scales, g_send, g_recv, n_send, n_recv, m_send, m_recv, s_send, s_recv, t_send, t_recv,
):
    loads = [
        pltpu.make_async_copy(src, dst, in_sem.at[i])
        for i, (src, dst) in enumerate(
            ((bcol_h, bcol), (ens_h, ens), (w_h, w), (prec_h, prec), (innov_h, innov), (nbs_h, nbs))
        )
    ]
    for load in loads:
        load.start()
    ia, jb = lax.axis_index("lat"), lax.axis_index("lon")
    up, down = lax.rem(ia + na - 1, na), lax.rem(ia + 1, na)
    west, east = lax.rem(jb + nb - 1, nb), lax.rem(jb + 1, nb)

    barrier = pltpu.get_barrier_semaphore()
    for peer in ((up, jb), (down, jb), (ia, west), (ia, east), (up, west), (down, east)):
        pl.semaphore_signal(barrier, inc=1, device_id=peer, device_id_type=MESH)

    def remote(src, dst, send, recv, peer):
        return pltpu.make_async_remote_copy(
            src_ref=src, dst_ref=dst, send_sem=send, recv_sem=recv, device_id=peer, device_id_type=MESH
        )

    lane1 = lax.broadcasted_iota(jnp.int32, (1, 128), 1)
    left_f = (lane1 < 64).astype(F32)
    left, right = left_f.astype(BF16), (1.0 - left_f).astype(BF16)
    row128 = lax.broadcasted_iota(jnp.int32, (128, 128), 0)
    lane128 = lax.broadcasted_iota(jnp.int32, (128, 128), 1)
    averager = jnp.where(row128 // 64 == lane128 // 64, 1.0 / K, 0.0).astype(BF16)

    for load in loads:
        load.wait()

    code = jnp.zeros((1, 128), jnp.int32)
    columns = jnp.concatenate([bcol[...], jnp.zeros((1, 128 - NBLK), jnp.int32)], 1)
    live = (lane1 < cnt[0, 0]) & (lane1 < NBLK)
    code = jnp.where(live, columns + 1, 0)
    msend[0] = jnp.broadcast_to(code, (8, 128))
    msend[1] = jnp.broadcast_to(pltpu.roll(code, 2 * NBLK, 1), (8, 128))
    code_own = pltpu.roll(code, NBLK, 1)
    for to, start, rows in ((0, 0, 8), (8, 8, 1), (9, 16, 1), (10, 24, 1), (11, 9, 7), (18, 17, 7), (25, 25, 7)):
        nbp[1, to : to + rows, 0:NNB] = nbs[start : start + rows]

    chosen = jnp.where(row128 == jnp.broadcast_to(columns, (128, 128)), 1.0, 0.0)
    chosen = jnp.where(lane128 < NBLK, chosen, 0.0)
    chosen = jnp.transpose(chosen)[:NBLK].astype(BF16)
    state = ens[...].reshape(CLAT * CLON, LEV * K)
    picked = dot(chosen, state)
    stacked = jnp.concatenate([picked[:, 128 * t : 128 * (t + 1)] for t in range(16)], 0)
    anomaly = stacked - dot(stacked.astype(BF16), averager)
    for t in range(16):
        part = anomaly[NBLK * t : NBLK * (t + 1)]
        sa[pl.ds(2 * t * PAD, NBLK), :] = part
        sa[pl.ds((2 * t + 1) * PAD, NBLK), :] = pltpu.roll(part, 64, 1)
    sp[0] = jnp.sqrt(prec[...].astype(F32))
    sp[1] = innov[...].astype(F32) * sp[0]

    U1, U2, REP = 32, 32, 1

    def observed(step, carry):
        for i in range(U1):
            b = lax.rem(step, 32 // U1) * U1 + i
            x = sa[pl.ds(b, LEV, stride=PAD), :][:, :K].astype(BF16)
            y = lax.dot_general(x, w[b], (((0,), (0,)), ((), ())), preferred_element_type=F32)
            yb[b, 0:K] = (y * sp[0, pl.ds(b, 1), :]).astype(BF16)
            forced = sp[1, pl.ds(b, 1), :]
            yb[b, K : K + 16] = jnp.where(lax.broadcasted_iota(jnp.int32, (16, 128), 0) == 0, forced, 0.0).astype(BF16)
        return carry

    def squared(step, carry):
        for i in range(U2):
            b = lax.rem(step, 32 // U2) * U2 + i
            g = lax.dot_general(yb[b], yb[b, 0:K], (((1,), (1,)), ((), ())), preferred_element_type=F32)
            sg[pl.ds(b, 72, stride=PAD), 0:K] = g[:72]
        return carry

    lax.fori_loop(0, 32 // U1 * REP, observed, 0)
    lax.fori_loop(0, 32 // U2 * REP, squared, 0)

    wide = lax.broadcasted_iota(jnp.int32, (NBLK, 128), 1)
    def unit(k):
        return sg[pl.ds(k * PAD, NBLK), :]

    for i in range(16):
        k = i + 16
        low = unit(i) if i == 0 else jnp.where(wide >= i, unit(i), pltpu.roll(unit(63 - i), 64 + i, 1))
        high = jnp.where(wide >= 64 + k, pltpu.roll(unit(k), 64, 1), pltpu.roll(unit(63 - k), k, 1))
        gall[1, i] = jnp.where(wide < 64, low, high).astype(BF16)
    spine = jnp.zeros((NBLK, 128), F32)
    for k in range(32, 64):
        spine = jnp.where(wide == k, unit(k), spine)
    gall[1, 16] = jnp.where(wide < 64, unit(64), pltpu.roll(spine, 64, 1)).astype(BF16)

    pl.semaphore_wait(barrier, 6)
    facts = [
        remote(nbp.at[1], nbp.at[0], n_send.at[0], n_recv.at[0], (up, jb)),
        remote(nbp.at[1], nbp.at[2], n_send.at[1], n_recv.at[1], (down, jb)),
        remote(msend.at[0], mrecv.at[0], m_send.at[0], m_recv.at[0], (ia, east)),
        remote(msend.at[1], mrecv.at[1], m_send.at[1], m_recv.at[1], (ia, west)),
    ]
    first = []
    for n, (lo, hi) in enumerate(CHUNKS):
        span = pl.ds(lo, hi - lo)
        first.append(
            [
                remote(gall.at[1, span], gall.at[0, span], g_send.at[0, n], g_recv.at[0, n], (ia, east)),
                remote(gall.at[1, span], gall.at[2, span], g_send.at[1, n], g_recv.at[1, n], (ia, west)),
            ]
        )
    for copy in facts + [copy for pair in first for copy in pair]:
        copy.start()

    def columns_of(r, carry):
        x = jnp.concatenate([ens[r, :, 128 * t : 128 * (t + 1)] for t in range(16)], 0)
        spread = (x.astype(F32) - dot(x, averager)).astype(BF16).astype(F32)
        for t in range(16):
            sx[r, pl.ds(t * 17, CLON), :] = spread[CLON * t : CLON * (t + 1)]
        for c in range(CLON):
            xa[r * CLON + c] = sx[r, pl.ds(c, 16, stride=17), :].astype(BF16)
        return carry

    lax.fori_loop(0, CLAT, columns_of, 0)

    for copy in facts:
        copy.wait()
    code3 = mrecv[0, 0:1, :] + code_own + mrecv[1, 0:1, :]
    is_live = (code3 > 0).astype(F32)
    place = jnp.maximum(code3 - 1, 0)
    b_row = (place // CLON).astype(F32)
    b_col = (place % CLON + (lane1 // NBLK - 1) * CLON).astype(F32)
    point = lax.broadcasted_iota(jnp.int32, (32, 128), 0)
    point = jnp.where(
        point < 8,
        point,
        jnp.where(point < 11, 8 * (point - 7), jnp.where(point < 18, point - 2, jnp.where(point < 25, point - 1, point))),
    )
    p_row = (2 * (point // 8)).astype(F32)
    p_col = (2 * (point % 8)).astype(F32)
    weights = []
    for u in (-1, 0, 1):
        listed = nbp[u + 1]
        count = jnp.zeros((32, 128), F32)
        for n in range(NNB):
            count += (listed[:, n : n + 1] - 96 * (u + 1) == wide).astype(F32)
        dlat = (b_row + float(u * CLAT)) - p_row
        dlon = b_col - p_col
        taper = jnp.exp(-(dlat * dlat + dlon * dlon) / (2.0 * LOC * LOC))
        valid = ((ia - u >= 0) & (ia - u < na)).astype(F32)
        weights.append(jnp.where(wide < 96, count * taper * is_live * valid, 0.0))
    whi, wlo = split(jnp.concatenate(weights, 0))
    lhs = jnp.concatenate([whi, wlo], 0)[:, :96]

    second = []
    for n, (lo, hi) in enumerate(CHUNKS):
        for copy in first[n]:
            copy.wait()
        for t in range(lo, hi, 2):
            ts = range(t, min(t + 2, hi))
            rhs = jnp.concatenate([jnp.concatenate([gall[v, i] for i in ts], 1) for v in range(3)], 0)
            o = dot(lhs, rhs)
            o = o[:96] + o[96:]
            for i in ts:
                part = o[:, 128 * (i - t) : 128 * (i - t + 1)]
                ssend[0, i] = part[:32].astype(BF16)
                own[i] = part[32:64]
                ssend[1, i] = part[64:].astype(BF16)
        span = pl.ds(lo, hi - lo)
        pair = [
            remote(ssend.at[0, span], srecv.at[0, span], s_send.at[0, n], s_recv.at[0, n], (down, jb)),
            remote(ssend.at[1, span], srecv.at[1, span], s_send.at[1, n], s_recv.at[1, n], (up, jb)),
        ]
        for copy in pair:
            copy.start()
        second.append(pair)
    for n, (lo, hi) in enumerate(CHUNKS):
        for copy in second[n]:
            copy.wait()
        for i in range(lo, hi):
            tile = own[i] + srecv[0, i].astype(F32) + srecv[1, i].astype(F32)
            if i == 16:
                s2[pl.ds(64 * PAD, 32), :] = tile
                s2[pl.ds(65 * PAD, 32), :] = pltpu.roll(tile, 64, 1)
                continue
            k = i + 16
            s2[pl.ds(i * PAD, 32), :] = tile
            s2[pl.ds((63 - i) * PAD, 32), :] = pltpu.roll(tile, 64 - i, 1)
            s2[pl.ds(k * PAD, 32), :] = pltpu.roll(tile, 64, 1)
            s2[pl.ds((63 - k) * PAD, 32), :] = pltpu.roll(tile, 128 - k, 1)
    row64 = lax.broadcasted_iota(jnp.int32, (K, 256), 0)
    lane256 = lax.broadcasted_iota(jnp.int32, (K, 256), 1)
    eye = (lane256 % 64 == row64).astype(F32)
    ones = jnp.where(
        lax.broadcasted_iota(jnp.int32, (256, 256), 0) // 64 == lax.broadcasted_iota(jnp.int32, (256, 256), 1) // 64,
        1.0, 0.0,
    ).astype(BF16)
    half64 = lax.broadcasted_iota(jnp.int32, (K, 128), 1) < 64
    row_k = lax.broadcasted_iota(jnp.int32, (K, 128), 0)
    lane_k = lax.broadcasted_iota(jnp.int32, (K, 128), 1)
    above = (lane_k > row_k) & (lane_k < 64)
    first_diagonal = (lane_k == row_k) & (row_k < 32)
    last_diagonal = (lane_k == row_k) & (row_k >= 32)
    half1 = lane1 < 64
    row16 = lax.broadcasted_iota(jnp.int32, (16, 256), 0)

    def two_rows(x):
        hi = x.astype(BF16).astype(F32)
        return jnp.where(row16 == 0, hi, jnp.where(row16 == 1, x - hi, 0.0)).astype(BF16)

    def both(x):
        return jnp.concatenate(split(x), 0)

    def thrice(a, b_hi, b_lo):
        o = dot(both(a), diagonal(b_hi, left, right))
        return o[:K] + o[K:] + dot(a.astype(BF16), diagonal(b_lo, left, right))

    def symmetric(m):
        upper, own_diagonal = [], []
        for p in (2 * m, 2 * m + 1):
            v = s2[pl.ds(p, K, stride=PAD), :]
            d = jnp.broadcast_to(s2[pl.ds(65 * PAD + p, 1), :], (K, 128))
            upper.append(jnp.where(above, v, 0.0))
            own_diagonal.append(jnp.where(first_diagonal, v, jnp.where(last_diagonal, d, 0.0)))
        whole = jnp.transpose(jnp.concatenate(upper, 0))[:K]
        second_half = pltpu.roll(upper[1] + own_diagonal[1], 64, 1)
        return whole + jnp.where(half64, upper[0] + own_diagonal[0], second_half)

    def begin(g):
        parts, proj = [], []
        for m in (2 * g, 2 * g + 1):
            parts.append(symmetric(m))
            q0 = s2[pl.ds(64 * PAD + 2 * m, 1), :]
            q1 = s2[pl.ds(64 * PAD + 2 * m + 1, 1), :]
            proj.append(jnp.where(half1, q0, pltpu.roll(q1, 64, 1)))
        gram = jnp.concatenate(parts, 1) + (K - 1.0) * eye
        yf[g] = gram
        scales[g, 1:2] = jnp.concatenate(proj, 1)
        scales[g, 0:1] = jnp.sum(gram * gram, axis=0, keepdims=True)

    def first_step(g):
        gram, row = yf[g], scales[g, 1:2]
        sums = dot(two_rows(scales[g, 0:1]), ones)
        g_hi = gram.astype(BF16)
        o = dot(jnp.concatenate([g_hi, two_rows(row)], 0), diagonal(g_hi, left, right))
        inv = 1.0 / jnp.sqrt(sums[0:1] + sums[1:2])
        x = gram * inv
        yf[g] = 1.5 * x - (0.5 * inv * inv) * o[:K]
        zf[g] = 1.5 * eye - 0.5 * x
        scales[g, 0:1] = inv
        scales[g, 1:2] = 1.5 * row - 0.5 * inv * (o[K : K + 1] + o[K + 1 : K + 2])

    def advance(g, refine, keep_y=True):
        y, z, row, p = yf[g], zf[g], scales[g, 1:2], pf[g]
        p_hi, p_lo = split(p)
        top = [y.astype(BF16)] if keep_y else []
        parts = top + [z.astype(BF16), two_rows(row)]
        if refine:
            parts += ([split(y)[1]] if keep_y else []) + [split(z)[1]]
        o = dot(jnp.concatenate(parts, 0), diagonal(p_hi, left, right))
        n = K if keep_y else 0
        yp, zp, rp = o[:n], o[n : n + K], o[n + K : n + K + 1] + o[n + K + 1 : n + K + 2]
        if refine:
            m = n + K + 16
            e = dot(jnp.concatenate(parts[: len(top) + 2], 0), diagonal(p_lo, left, right))
            yp = yp + o[m : m + n] + e[:n]
            zp = zp + o[m + n : m + n + K] + e[n : n + K]
            rp = rp + e[n + K : n + K + 1]
        if keep_y:
            yf[g] = 1.5 * y - 0.5 * yp
        zf[g] = 1.5 * z - 0.5 * zp
        scales[g, 1:2] = 1.5 * row - 0.5 * rp

    def refined(g):
        pf[g] = thrice(zf[g], *split(yf[g]))

    def turn(step, carry):
        for g in range(8):
            pf[g] = dot(zf[g].astype(BF16), diagonal(yf[g].astype(BF16), left, right))
        for g in range(8):
            advance(g, False)
        return carry

    R4, R5 = 1, 1

    def last_turns(groups):
        for g in groups:
            refined(g)
        for g in groups:
            advance(g, R4)
        for g in groups:
            refined(g)
        for g in groups:
            advance(g, R5, False)
        for g in groups:
            z, inv = zf[g], scales[g, 0:1]
            s = dot(both(z * scales[g, 1:2]), ones)
            t = z * (jnp.sqrt(K - 1.0) * jnp.sqrt(inv)) + (s[:K] + s[K:]) * inv
            tb[2 * g] = t[:, :128].astype(BF16)
            tb[2 * g + 1] = t[:, 128:].astype(BF16)

    for g in range(8):
        begin(g)
    for g in range(8):
        first_step(g)
    lax.fori_loop(0, NSI - 3, turn, 0)
    last_turns(range(4))

    p0, p8, p10 = tb[0].astype(F32), tb[4].astype(F32), tb[5].astype(F32)
    csend[0] = jnp.where(half64, p0, pltpu.roll(p8, 64, 1)).astype(BF16)
    csend[1] = jnp.where(half64, pltpu.roll(p8, 64, 1), pltpu.roll(p10, 64, 1)).astype(BF16)
    third = [
        remote(tb.at[pl.ds(0, 4)], rrow, t_send.at[0], t_recv.at[0], (up, jb)),
        remote(csend, rcol, t_send.at[1], t_recv.at[1], (ia, west)),
        remote(csend.at[0], rcor, t_send.at[2], t_recv.at[2], (up, west)),
    ]
    for copy in third:
        copy.start()
    last_turns(range(4, 8))
    zero64 = jnp.zeros((K, 128), F32)

    def expand(pair):
        v = pair.astype(F32)
        r = pltpu.roll(v, 64, 1)
        d0 = jnp.concatenate([jnp.where(half64, v, zero64), jnp.where(half64, zero64, r)], 0)
        d1 = jnp.concatenate([jnp.where(half64, r, zero64), jnp.where(half64, zero64, v)], 0)
        return d0.astype(BF16), d1.astype(BF16)

    for m in range(16):
        for p, d in zip(ORDER[2 * m : 2 * m + 2], expand(tb[m])):
            dd[p // 8, p % 8] = d

    def finish(a):
        none = jnp.zeros((16, 128), BF16)
        for c in range(8):
            base = 2 * a * CLON + 2 * c
            ee, eo = xa[base], xa[base + 1] * 0.5
            oe, oo = xa[base + CLON] * 0.5, xa[base + CLON + 1] * 0.25
            lower = jnp.concatenate([jnp.concatenate([oe, none], 1), jnp.concatenate([oo, oo], 1)], 0)
            upper = jnp.concatenate([jnp.concatenate([ee, none], 1), jnp.concatenate([eo, eo], 1), lower], 0)
            o = dot(upper, dd[a, c : c + 2].reshape(256, 128))
            e = dot(lower, dd[a + 1, c : c + 2].reshape(256, 128))
            so[0, pl.ds(2 * c, 16, stride=17), :] = o[0:16]
            so[0, pl.ds(2 * c + 1, 16, stride=17), :] = o[16:32]
            so[1, pl.ds(2 * c, 16, stride=17), :] = o[32:48] + e[0:16]
            so[1, pl.ds(2 * c + 1, 16, stride=17), :] = o[48:64] + e[16:32]
        for i in range(2):
            r = 2 * a + i
            x = jnp.concatenate([ens[r, :, 128 * t : 128 * (t + 1)] for t in range(16)], 0)
            center = dot(x, averager)
            for t in range(16):
                rows = so[i, pl.ds(t * 17, CLON), :] + center[CLON * t : CLON * (t + 1)]
                out[r, :, 128 * t : 128 * (t + 1)] = rows.astype(BF16)

    def drain(a):
        return pltpu.make_async_copy(out_v.at[pl.ds(2 * a, 2)], out.at[pl.ds(2 * a, 2)], o_sem.at[a])

    third[1].wait()
    for i in range(2):
        for p, d in zip(((0, 1), (2, 3))[i], expand(rcol[i])):
            dd[p, 8] = d

    def most(a, carry):
        finish(a)
        return carry

    lax.fori_loop(0, 3, most, 0)
    third[0].wait()
    third[2].wait()
    edge = (ia == na - 1).astype(F32)
    for i in range(4):
        for c, d in zip((2 * i, 2 * i + 1), expand(rrow[i])):
            dd[4, c] = (d.astype(F32) * (1.0 - edge) + dd[3, c].astype(F32) * edge).astype(BF16)
    bottom = pltpu.roll(rcol[1].astype(F32), 64, 1)
    dd[4, 8] = expand(rcor[...].astype(F32) * (1.0 - edge) + bottom * edge)[0]
    finish(3)


def solution(mesh):
    na, nb = mesh.shape["lat"], mesh.shape["lon"]

    def body(ensemble, channel_weights, block_column, innovation, error_precision, block_count, neighbours):
        dma = pltpu.SemaphoreType.DMA
        return pl.pallas_call(
            functools.partial(kernel, na, nb),
            out_shape=jax.ShapeDtypeStruct(ensemble.shape, BF16),
            in_specs=[pl.BlockSpec(memory_space=pltpu.SMEM if i == 5 else pltpu.HBM) for i in range(7)],
            out_specs=pl.BlockSpec(memory_space=pltpu.VMEM),
            scratch_shapes=[
                pltpu.VMEM(ensemble.shape, BF16),
                dma((4,)),
                pltpu.VMEM((8, K, 256), F32),
                pltpu.VMEM((8, K, 256), F32),
                pltpu.VMEM(ensemble.shape, BF16),
                pltpu.VMEM((NBLK, LEV, OB), BF16),
                pltpu.VMEM((1, NBLK), jnp.int32),
                pltpu.VMEM((NBLK, OB), BF16),
                pltpu.VMEM((NBLK, OB), BF16),
                pltpu.VMEM((32, NNB), jnp.int32),
                dma((6,)),
                pltpu.VMEM((NBLK, K + 16, OB), BF16),
                pltpu.VMEM((LEV * PAD, 128), F32),
                pltpu.VMEM((72 * PAD, 128), F32),
                pltpu.VMEM((2, NBLK, OB), F32),
                pltpu.VMEM((3, NT, NBLK, 128), BF16),
                pltpu.VMEM((3, 32, 128), jnp.int32),
                pltpu.VMEM((2, 8, 128), jnp.int32),
                pltpu.VMEM((2, 8, 128), jnp.int32),
                pltpu.VMEM((2, NT, 32, 128), BF16),
                pltpu.VMEM((2, NT, 32, 128), BF16),
                pltpu.VMEM((NT, 32, 128), F32),
                pltpu.VMEM((66 * PAD, 128), F32),
                pltpu.VMEM((8, K, 256), F32),
                pltpu.VMEM((16, K, 128), BF16),
                pltpu.VMEM((2, K, 128), BF16),
                pltpu.VMEM((4, K, 128), BF16),
                pltpu.VMEM((2, K, 128), BF16),
                pltpu.VMEM((K, 128), BF16),
                pltpu.VMEM((5, 9, 128, 128), BF16),
                pltpu.VMEM((CLAT * CLON, 16, 128), BF16),
                pltpu.VMEM((CLAT, 272, 128), F32),
                pltpu.VMEM((2, 272, 128), F32),
                pltpu.VMEM((8, 8, 256), F32),
                dma((2, 4)), dma((2, 4)), dma((2,)), dma((2,)), dma((2,)), dma((2,)),
                dma((2, 4)), dma((2, 4)), dma((3,)), dma((3,)),
            ],
            compiler_params=pltpu.CompilerParams(
                collective_id=0, has_side_effects=True, vmem_limit_bytes=20 * 2**20
            ),
        )(
            *(
                x if x.ndim == 2 and x.shape[1] == 1 else pltpu.with_memory_space_constraint(x, pltpu.HBM)
                for x in (
                    ensemble,
                    channel_weights[0, 0],
                    block_column[0],
                    innovation[0, 0],
                    error_precision[0, 0],
                    block_count,
                    neighbours.reshape(32, NNB),
                )
            )
        )

    return jax.shard_map(
        body,
        mesh=mesh,
        in_specs=(
            P("lat", "lon", None),
            P("lat", "lon", None, None, None),
            P("lat", "lon", None),
            P("lat", "lon", None, None),
            P("lat", "lon", None, None),
            P("lat", "lon"),
            P("lat", "lon", None),
        ),
        out_specs=P("lat", "lon", None),
        check_vma=False,
    )
```

```python
import functools

import jax
import jax.numpy as jnp
from jax import lax
from jax.experimental import pallas as pl
from jax.experimental.pallas import tpu as pltpu
from jax.sharding import PartitionSpec as P

F32 = jnp.float32
BF16 = jnp.bfloat16
MESH = pl.DeviceIdType.MESH
NSI = 6
LOC = 12
K = 64
OB = 128
CLAT = 8
CLON = 16
NBLK = 32
NNB = 12
LEV = 32
NT = 17
PAD = 33
CHUNKS = ((0, 4), (4, 8), (8, 12), (12, 17))
ORDER = (0, 1, 2, 3, 4, 5, 6, 7, 8, 16, 24, 9, 10, 11, 12, 13, 14, 15) + tuple(range(17, 24)) + tuple(range(25, 32))


def dot(a, b):
    return jnp.dot(a, b, preferred_element_type=F32)


def split(x):
    hi = x.astype(BF16)
    return hi, (x - hi.astype(F32)).astype(BF16)


def diagonal(x, left, right):
    first, second = x[:, :128], x[:, 128:]
    zero = jnp.zeros_like(first)
    return jnp.concatenate(
        [
            jnp.concatenate([first * left, zero], 1),
            jnp.concatenate([first * right, zero], 1),
            jnp.concatenate([zero, second * left], 1),
            jnp.concatenate([zero, second * right], 1),
        ],
        0,
    )


def kernel(
    na, nb, ens_h, w_h, bcol_h, innov_h, prec_h, cnt, nbs_h, out,
    out_v, o_sem, pf, yf, ens, w, bcol, innov, prec, nbs, in_sem, yb, sa, sg, sp, gall, nbp, msend, mrecv, ssend, srecv, own, s2, zf, tb, csend, rrow, rcol, rcor, dd, xa, sx, so,
    scales, g_send, g_recv, n_send, n_recv, m_send, m_recv, s_send, s_recv, t_send, t_recv,
):
    loads = [
        pltpu.make_async_copy(src, dst, in_sem.at[i])
        for i, (src, dst) in enumerate(
            ((bcol_h, bcol), (ens_h, ens), (prec_h, prec), (innov_h, innov), (w_h, w), (nbs_h, nbs))
        )
    ]
    for load in loads:
        load.start()
    ia, jb = lax.axis_index("lat"), lax.axis_index("lon")
    up, down = lax.rem(ia + na - 1, na), lax.rem(ia + 1, na)
    west, east = lax.rem(jb + nb - 1, nb), lax.rem(jb + 1, nb)

    has_up, has_down = ia > 0, ia < na - 1

    barrier = pltpu.get_barrier_semaphore()

    def greet(peers):
        for peer in peers:
            pl.semaphore_signal(barrier, inc=1, device_id=peer, device_id_type=MESH)

    greet(((ia, west), (ia, east)))
    pl.when(has_up)(lambda: greet(((up, jb), (up, west))))
    pl.when(has_down)(lambda: greet(((down, jb), (down, east))))

    @pl.when(jnp.logical_not(has_up))
    def _():
        srecv[0] = jnp.zeros_like(srecv[0])
        nbp[2] = jnp.zeros_like(nbp[2])

    @pl.when(jnp.logical_not(has_down))
    def _():
        srecv[1] = jnp.zeros_like(srecv[1])
        nbp[0] = jnp.zeros_like(nbp[0])
        rrow[...] = jnp.zeros_like(rrow)
        rcor[...] = jnp.zeros_like(rcor)

    def each(cond, copies, what):
        def run():
            for copy in copies:
                getattr(copy, what)()

        pl.when(cond)(run)

    def remote(src, dst, send, recv, peer):
        return pltpu.make_async_remote_copy(
            src_ref=src, dst_ref=dst, send_sem=send, recv_sem=recv, device_id=peer, device_id_type=MESH
        )

    lane1 = lax.broadcasted_iota(jnp.int32, (1, 128), 1)
    left_f = (lane1 < 64).astype(F32)
    left, right = left_f.astype(BF16), (1.0 - left_f).astype(BF16)
    row128 = lax.broadcasted_iota(jnp.int32, (128, 128), 0)
    lane128 = lax.broadcasted_iota(jnp.int32, (128, 128), 1)
    averager = jnp.where(row128 // 64 == lane128 // 64, 1.0 / K, 0.0).astype(BF16)

    loads[0].wait()
    loads[1].wait()

    code = jnp.zeros((1, 128), jnp.int32)
    columns = jnp.concatenate([bcol[...], jnp.zeros((1, 128 - NBLK), jnp.int32)], 1)
    live = (lane1 < cnt[0, 0]) & (lane1 < NBLK)
    code = jnp.where(live, columns + 1, 0)
    msend[0] = jnp.broadcast_to(code, (8, 128))
    msend[1] = jnp.broadcast_to(pltpu.roll(code, 2 * NBLK, 1), (8, 128))
    code_own = pltpu.roll(code, NBLK, 1)

    chosen = jnp.where(row128 == jnp.broadcast_to(columns, (128, 128)), 1.0, 0.0)
    chosen = jnp.where(lane128 < NBLK, chosen, 0.0)
    chosen = jnp.transpose(chosen)[:NBLK].astype(BF16)
    state = ens[...].reshape(CLAT * CLON, LEV * K)
    picked = dot(chosen, state)
    stacked = jnp.concatenate([picked[:, 128 * t : 128 * (t + 1)] for t in range(16)], 0)
    anomaly = stacked - dot(stacked.astype(BF16), averager)
    for t in range(16):
        part = anomaly[NBLK * t : NBLK * (t + 1)]
        sa[pl.ds(2 * t * PAD, NBLK), :] = part
        sa[pl.ds((2 * t + 1) * PAD, NBLK), :] = pltpu.roll(part, 64, 1)
    for load in loads[2:5]:
        load.wait()
    sp[0] = jnp.sqrt(prec[...].astype(F32))
    sp[1] = innov[...].astype(F32) * sp[0]

    U1, U2, REP = 32, 32, 1

    def observed(step, carry):
        for i in range(U1):
            b = lax.rem(step, 32 // U1) * U1 + i
            x = sa[pl.ds(b, LEV, stride=PAD), :][:, :K].astype(BF16)
            y = lax.dot_general(x, w[b], (((0,), (0,)), ((), ())), preferred_element_type=F32)
            yb[b, 0:K] = (y * sp[0, pl.ds(b, 1), :]).astype(BF16)
            forced = sp[1, pl.ds(b, 1), :]
            yb[b, K : K + 16] = jnp.where(lax.broadcasted_iota(jnp.int32, (16, 128), 0) == 0, forced, 0.0).astype(BF16)
        return carry

    def squared(step, carry):
        for i in range(U2):
            b = lax.rem(step, 32 // U2) * U2 + i
            g = lax.dot_general(yb[b], yb[b, 0:K], (((1,), (1,)), ((), ())), preferred_element_type=F32)
            sg[pl.ds(b, 72, stride=PAD), 0:K] = g[:72]
        return carry

    lax.fori_loop(0, 32 // U1 * REP, observed, 0)
    lax.fori_loop(0, 32 // U2 * REP, squared, 0)

    wide = lax.broadcasted_iota(jnp.int32, (NBLK, 128), 1)
    def unit(k):
        return sg[pl.ds(k * PAD, NBLK), :]

    def pack(i):
        if i == 16:
            spine = jnp.zeros((NBLK, 128), F32)
            for k in range(32, 64):
                spine = jnp.where(wide == k, unit(k), spine)
            gall[1, 16] = jnp.where(wide < 64, unit(64), pltpu.roll(spine, 64, 1)).astype(BF16)
            return
        k = i + 16
        low = unit(i) if i == 0 else jnp.where(wide >= i, unit(i), pltpu.roll(unit(63 - i), 64 + i, 1))
        high = jnp.where(wide >= 64 + k, pltpu.roll(unit(k), 64, 1), pltpu.roll(unit(63 - k), k, 1))
        gall[1, i] = jnp.where(wide < 64, low, high).astype(BF16)

    loads[5].wait()
    for to, start, rows in ((0, 0, 8), (8, 8, 1), (9, 16, 1), (10, 24, 1), (11, 9, 7), (18, 17, 7), (25, 25, 7)):
        nbp[1, to : to + rows, 0:NNB] = nbs[start : start + rows]
    pl.semaphore_wait(barrier, 2 + 2 * has_up.astype(jnp.int32) + 2 * has_down.astype(jnp.int32))
    facts = [
        remote(nbp.at[1], nbp.at[0], n_send.at[0], n_recv.at[0], (up, jb)),
        remote(nbp.at[1], nbp.at[2], n_send.at[1], n_recv.at[1], (down, jb)),
        remote(msend.at[0], mrecv.at[0], m_send.at[0], m_recv.at[0], (ia, east)),
        remote(msend.at[1], mrecv.at[1], m_send.at[1], m_recv.at[1], (ia, west)),
    ]
    each(has_up, facts[:1], "start")
    each(has_down, facts[1:2], "start")
    for copy in facts[2:]:
        copy.start()
    for i in range(17):
        pack(i)
    first = []
    for n, (lo, hi) in enumerate(CHUNKS):
        span = pl.ds(lo, hi - lo)
        pair = [
            remote(gall.at[1, span], gall.at[0, span], g_send.at[0, n], g_recv.at[0, n], (ia, east)),
            remote(gall.at[1, span], gall.at[2, span], g_send.at[1, n], g_recv.at[1, n], (ia, west)),
        ]
        for copy in pair:
            copy.start()
        first.append(pair)

    def columns_of(r, carry):
        x = jnp.concatenate([ens[r, :, 128 * t : 128 * (t + 1)] for t in range(16)], 0)
        spread = (x.astype(F32) - dot(x, averager)).astype(BF16).astype(F32)
        for t in range(16):
            sx[r, pl.ds(t * 17, CLON), :] = spread[CLON * t : CLON * (t + 1)]
        for c in range(CLON):
            xa[r * CLON + c] = sx[r, pl.ds(c, 16, stride=17), :].astype(BF16)
        return carry

    lax.fori_loop(0, CLAT, columns_of, 0)

    each(has_down, facts[:1], "wait_recv")
    each(has_up, facts[1:2], "wait_recv")
    for copy in facts[2:]:
        copy.wait_recv()
    code3 = mrecv[0, 0:1, :] + code_own + mrecv[1, 0:1, :]
    is_live = (code3 > 0).astype(F32)
    place = jnp.maximum(code3 - 1, 0)
    b_row = (place // CLON).astype(F32)
    b_col = (place % CLON + (lane1 // NBLK - 1) * CLON).astype(F32)
    point = lax.broadcasted_iota(jnp.int32, (32, 128), 0)
    point = jnp.where(
        point < 8,
        point,
        jnp.where(point < 11, 8 * (point - 7), jnp.where(point < 18, point - 2, jnp.where(point < 25, point - 1, point))),
    )
    p_row = (2 * (point // 8)).astype(F32)
    p_col = (2 * (point % 8)).astype(F32)
    weights = []
    for u in (-1, 0, 1):
        listed = nbp[u + 1]
        count = jnp.zeros((32, 128), F32)
        for n in range(NNB):
            count += (listed[:, n : n + 1] - 96 * (u + 1) == wide).astype(F32)
        dlat = (b_row + float(u * CLAT)) - p_row
        dlon = b_col - p_col
        taper = jnp.exp(-(dlat * dlat + dlon * dlon) / (2.0 * LOC * LOC))
        valid = ((ia - u >= 0) & (ia - u < na)).astype(F32)
        weights.append(jnp.where(wide < 96, count * taper * is_live * valid, 0.0))
    whi, wlo = split(jnp.concatenate(weights, 0))
    lhs = jnp.concatenate([whi, wlo], 0)[:, :96]

    second = []
    for n, (lo, hi) in enumerate(CHUNKS):
        for copy in first[n]:
            copy.wait_recv()
        for t in range(lo, hi, 2):
            ts = range(t, min(t + 2, hi))
            rhs = jnp.concatenate([jnp.concatenate([gall[v, i] for i in ts], 1) for v in range(3)], 0)
            o = dot(lhs, rhs)
            o = o[:96] + o[96:]
            for i in ts:
                part = o[:, 128 * (i - t) : 128 * (i - t + 1)]
                ssend[0, i] = part[:32].astype(BF16)
                own[i] = part[32:64]
                ssend[1, i] = part[64:].astype(BF16)
        span = pl.ds(lo, hi - lo)
        pair = [
            remote(ssend.at[0, span], srecv.at[0, span], s_send.at[0, n], s_recv.at[0, n], (down, jb)),
            remote(ssend.at[1, span], srecv.at[1, span], s_send.at[1, n], s_recv.at[1, n], (up, jb)),
        ]
        each(has_down, pair[:1], "start")
        each(has_up, pair[1:], "start")
        second.append(pair)
    for n, (lo, hi) in enumerate(CHUNKS):
        each(has_up, second[n][:1], "wait_recv")
        each(has_down, second[n][1:], "wait_recv")
        for i in range(lo, hi):
            tile = own[i] + srecv[0, i].astype(F32) + srecv[1, i].astype(F32)
            if i == 16:
                s2[pl.ds(64 * PAD, 32), :] = tile
                s2[pl.ds(65 * PAD, 32), :] = pltpu.roll(tile, 64, 1)
                continue
            k = i + 16
            s2[pl.ds(i * PAD, 32), :] = tile
            s2[pl.ds((63 - i) * PAD, 32), :] = pltpu.roll(tile, 64 - i, 1)
            s2[pl.ds(k * PAD, 32), :] = pltpu.roll(tile, 64, 1)
            s2[pl.ds((63 - k) * PAD, 32), :] = pltpu.roll(tile, 128 - k, 1)
    row64 = lax.broadcasted_iota(jnp.int32, (K, 256), 0)
    lane256 = lax.broadcasted_iota(jnp.int32, (K, 256), 1)
    eye = (lane256 % 64 == row64).astype(F32)
    ones = jnp.where(
        lax.broadcasted_iota(jnp.int32, (256, 256), 0) // 64 == lax.broadcasted_iota(jnp.int32, (256, 256), 1) // 64,
        1.0, 0.0,
    ).astype(BF16)
    half64 = lax.broadcasted_iota(jnp.int32, (K, 128), 1) < 64
    row_k = lax.broadcasted_iota(jnp.int32, (K, 128), 0)
    lane_k = lax.broadcasted_iota(jnp.int32, (K, 128), 1)
    above = (lane_k > row_k) & (lane_k < 64)
    first_diagonal = (lane_k == row_k) & (row_k < 32)
    last_diagonal = (lane_k == row_k) & (row_k >= 32)
    half1 = lane1 < 64
    row16 = lax.broadcasted_iota(jnp.int32, (16, 256), 0)

    def two_rows(x):
        hi = x.astype(BF16).astype(F32)
        return jnp.where(row16 == 0, hi, jnp.where(row16 == 1, x - hi, 0.0)).astype(BF16)

    def both(x):
        return jnp.concatenate(split(x), 0)

    def thrice(a, b_hi, b_lo):
        o = dot(both(a), diagonal(b_hi, left, right))
        return o[:K] + o[K:] + dot(a.astype(BF16), diagonal(b_lo, left, right))

    def symmetric(m):
        upper, own_diagonal = [], []
        for p in (2 * m, 2 * m + 1):
            v = s2[pl.ds(p, K, stride=PAD), :]
            d = jnp.broadcast_to(s2[pl.ds(65 * PAD + p, 1), :], (K, 128))
            upper.append(jnp.where(above, v, 0.0))
            own_diagonal.append(jnp.where(first_diagonal, v, jnp.where(last_diagonal, d, 0.0)))
        whole = jnp.transpose(jnp.concatenate(upper, 0))[:K]
        second_half = pltpu.roll(upper[1] + own_diagonal[1], 64, 1)
        return whole + jnp.where(half64, upper[0] + own_diagonal[0], second_half)

    def begin(g):
        parts, proj = [], []
        for m in (2 * g, 2 * g + 1):
            parts.append(symmetric(m))
            q0 = s2[pl.ds(64 * PAD + 2 * m, 1), :]
            q1 = s2[pl.ds(64 * PAD + 2 * m + 1, 1), :]
            proj.append(jnp.where(half1, q0, pltpu.roll(q1, 64, 1)))
        gram = jnp.concatenate(parts, 1) + (K - 1.0) * eye
        yf[g] = gram
        scales[g, 1:2] = jnp.concatenate(proj, 1)
        scales[g, 0:1] = jnp.sum(gram * gram, axis=0, keepdims=True)

    def first_step(g):
        gram, row = yf[g], scales[g, 1:2]
        sums = dot(two_rows(scales[g, 0:1]), ones)
        g_hi = gram.astype(BF16)
        o = dot(jnp.concatenate([g_hi, two_rows(row)], 0), diagonal(g_hi, left, right))
        inv = 1.0 / jnp.sqrt(sums[0:1] + sums[1:2])
        x = gram * inv
        yf[g] = 1.5 * x - (0.5 * inv * inv) * o[:K]
        zf[g] = 1.5 * eye - 0.5 * x
        scales[g, 0:1] = inv
        scales[g, 1:2] = 1.5 * row - 0.5 * inv * (o[K : K + 1] + o[K + 1 : K + 2])

    def advance(g, refine, keep_y=True):
        y, z, row, p = yf[g], zf[g], scales[g, 1:2], pf[g]
        p_hi, p_lo = split(p)
        top = [y.astype(BF16)] if keep_y else []
        parts = top + [z.astype(BF16), two_rows(row)]
        if refine:
            parts += ([split(y)[1]] if keep_y else []) + [split(z)[1]]
        o = dot(jnp.concatenate(parts, 0), diagonal(p_hi, left, right))
        n = K if keep_y else 0
        yp, zp, rp = o[:n], o[n : n + K], o[n + K : n + K + 1] + o[n + K + 1 : n + K + 2]
        if refine:
            m = n + K + 16
            e = dot(jnp.concatenate(parts[: len(top) + 2], 0), diagonal(p_lo, left, right))
            yp = yp + o[m : m + n] + e[:n]
            zp = zp + o[m + n : m + n + K] + e[n : n + K]
            rp = rp + e[n + K : n + K + 1]
        if keep_y:
            yf[g] = 1.5 * y - 0.5 * yp
        zf[g] = 1.5 * z - 0.5 * zp
        scales[g, 1:2] = 1.5 * row - 0.5 * rp

    def refined(g):
        pf[g] = thrice(zf[g], *split(yf[g]))

    def turn(step, carry):
        for g in range(8):
            pf[g] = dot(zf[g].astype(BF16), diagonal(yf[g].astype(BF16), left, right))
        for g in range(8):
            advance(g, False)
        return carry

    R4, R5 = 1, 1

    def last_turns(groups):
        for g in groups:
            refined(g)
        for g in groups:
            advance(g, R4)
        for g in groups:
            refined(g)
        for g in groups:
            advance(g, R5, False)
        for g in groups:
            z, inv = zf[g], scales[g, 0:1]
            s = dot(both(z * scales[g, 1:2]), ones)
            t = z * (jnp.sqrt(K - 1.0) * jnp.sqrt(inv)) + (s[:K] + s[K:]) * inv
            tb[2 * g] = t[:, :128].astype(BF16)
            tb[2 * g + 1] = t[:, 128:].astype(BF16)

    for g in range(8):
        begin(g)
    for g in range(8):
        first_step(g)
    lax.fori_loop(0, NSI - 3, turn, 0)
    EG = 4
    last_turns(range(EG))

    third = [
        remote(tb.at[pl.ds(0, 4)], rrow, t_send.at[0], t_recv.at[0], (up, jb)),
        remote(csend, rcol, t_send.at[1], t_recv.at[1], (ia, west)),
        remote(tb.at[0], rcor, t_send.at[2], t_recv.at[2], (up, west)),
    ]
    p0, p8, p10 = tb[0].astype(F32), tb[4].astype(F32), tb[5].astype(F32)
    csend[0] = jnp.where(half64, p0, pltpu.roll(p8, 64, 1)).astype(BF16)
    csend[1] = jnp.where(half64, pltpu.roll(p8, 64, 1), pltpu.roll(p10, 64, 1)).astype(BF16)
    third[1].start()
    each(has_up, third[::2], "start")
    last_turns(range(EG, 8))
    zero64 = jnp.zeros((K, 128), F32)

    def expand(pair):
        v = pair.astype(F32)
        r = pltpu.roll(v, 64, 1)
        d0 = jnp.concatenate([jnp.where(half64, v, zero64), jnp.where(half64, zero64, r)], 0)
        d1 = jnp.concatenate([jnp.where(half64, r, zero64), jnp.where(half64, zero64, v)], 0)
        return d0.astype(BF16), d1.astype(BF16)

    for m in range(16):
        for p, d in zip(ORDER[2 * m : 2 * m + 2], expand(tb[m])):
            dd[p // 8, p % 8] = d

    def finish(a):
        none = jnp.zeros((16, 128), BF16)
        for c in range(8):
            base = 2 * a * CLON + 2 * c
            ee, eo = xa[base], xa[base + 1] * 0.5
            oe, oo = xa[base + CLON] * 0.5, xa[base + CLON + 1] * 0.25
            lower = jnp.concatenate([jnp.concatenate([oe, none], 1), jnp.concatenate([oo, oo], 1)], 0)
            upper = jnp.concatenate([jnp.concatenate([ee, none], 1), jnp.concatenate([eo, eo], 1), lower], 0)
            o = dot(upper, dd[a, c : c + 2].reshape(256, 128))
            e = dot(lower, dd[a + 1, c : c + 2].reshape(256, 128))
            so[0, pl.ds(2 * c, 16, stride=17), :] = o[0:16]
            so[0, pl.ds(2 * c + 1, 16, stride=17), :] = o[16:32]
            so[1, pl.ds(2 * c, 16, stride=17), :] = o[32:48] + e[0:16]
            so[1, pl.ds(2 * c + 1, 16, stride=17), :] = o[48:64] + e[16:32]
        for i in range(2):
            r = 2 * a + i
            x = jnp.concatenate([ens[r, :, 128 * t : 128 * (t + 1)] for t in range(16)], 0)
            center = dot(x, averager)
            for t in range(16):
                rows = so[i, pl.ds(t * 17, CLON), :] + center[CLON * t : CLON * (t + 1)]
                out[r, :, 128 * t : 128 * (t + 1)] = rows.astype(BF16)

    def drain(a):
        return pltpu.make_async_copy(out_v.at[pl.ds(2 * a, 2)], out.at[pl.ds(2 * a, 2)], o_sem.at[a])

    third[1].wait_recv()
    for i in range(2):
        for p, d in zip(((0, 1), (2, 3))[i], expand(rcol[i])):
            dd[p, 8] = d

    def most(a, carry):
        finish(a)
        return carry

    lax.fori_loop(0, 3, most, 0)
    each(has_down, third[::2], "wait_recv")
    edge = (ia == na - 1).astype(F32)
    for i in range(4):
        for c, d in zip((2 * i, 2 * i + 1), expand(rrow[i])):
            dd[4, c] = (d.astype(F32) * (1.0 - edge) + dd[3, c].astype(F32) * edge).astype(BF16)
    bottom = pltpu.roll(rcol[1].astype(F32), 64, 1)
    dd[4, 8] = expand(rcor[...].astype(F32) * (1.0 - edge) + bottom * edge)[0]
    finish(3)
    for copy in facts[2:] + third[1:2] + [copy for pair in first for copy in pair]:
        copy.wait_send()
    each(has_up, facts[:1] + third[::2] + [pair[1] for pair in second], "wait_send")
    each(has_down, facts[1:2] + [pair[0] for pair in second], "wait_send")


def solution(mesh):
    na, nb = mesh.shape["lat"], mesh.shape["lon"]

    def body(ensemble, channel_weights, block_column, innovation, error_precision, block_count, neighbours):
        dma = pltpu.SemaphoreType.DMA
        return pl.pallas_call(
            functools.partial(kernel, na, nb),
            out_shape=jax.ShapeDtypeStruct(ensemble.shape, BF16),
            in_specs=[pl.BlockSpec(memory_space=pltpu.SMEM if i == 5 else pltpu.HBM) for i in range(7)],
            out_specs=pl.BlockSpec(memory_space=pltpu.VMEM),
            scratch_shapes=[
                pltpu.VMEM(ensemble.shape, BF16),
                dma((4,)),
                pltpu.VMEM((8, K, 256), F32),
                pltpu.VMEM((8, K, 256), F32),
                pltpu.VMEM(ensemble.shape, BF16),
                pltpu.VMEM((NBLK, LEV, OB), BF16),
                pltpu.VMEM((1, NBLK), jnp.int32),
                pltpu.VMEM((NBLK, OB), BF16),
                pltpu.VMEM((NBLK, OB), BF16),
                pltpu.VMEM((32, NNB), jnp.int32),
                dma((6,)),
                pltpu.VMEM((NBLK, K + 16, OB), BF16),
                pltpu.VMEM((LEV * PAD, 128), F32),
                pltpu.VMEM((72 * PAD, 128), F32),
                pltpu.VMEM((2, NBLK, OB), F32),
                pltpu.VMEM((3, NT, NBLK, 128), BF16),
                pltpu.VMEM((3, 32, 128), jnp.int32),
                pltpu.VMEM((2, 8, 128), jnp.int32),
                pltpu.VMEM((2, 8, 128), jnp.int32),
                pltpu.VMEM((2, NT, 32, 128), BF16),
                pltpu.VMEM((2, NT, 32, 128), BF16),
                pltpu.VMEM((NT, 32, 128), F32),
                pltpu.VMEM((66 * PAD, 128), F32),
                pltpu.VMEM((8, K, 256), F32),
                pltpu.VMEM((16, K, 128), BF16),
                pltpu.VMEM((2, K, 128), BF16),
                pltpu.VMEM((4, K, 128), BF16),
                pltpu.VMEM((2, K, 128), BF16),
                pltpu.VMEM((K, 128), BF16),
                pltpu.VMEM((5, 9, 128, 128), BF16),
                pltpu.VMEM((CLAT * CLON, 16, 128), BF16),
                pltpu.VMEM((CLAT, 272, 128), F32),
                pltpu.VMEM((2, 272, 128), F32),
                pltpu.VMEM((8, 8, 256), F32),
                dma((2, len(CHUNKS))), dma((2, len(CHUNKS))), dma((2,)), dma((2,)), dma((2,)), dma((2,)),
                dma((2, len(CHUNKS))), dma((2, len(CHUNKS))), dma((3,)), dma((3,)),
            ],
            compiler_params=pltpu.CompilerParams(
                collective_id=0, has_side_effects=True, vmem_limit_bytes=20 * 2**20
            ),
        )(
            *(
                x if x.ndim == 2 and x.shape[1] == 1 else pltpu.with_memory_space_constraint(x, pltpu.HBM)
                for x in (
                    ensemble,
                    channel_weights[0, 0],
                    block_column[0],
                    innovation[0, 0],
                    error_precision[0, 0],
                    block_count,
                    neighbours.reshape(32, NNB),
                )
            )
        )

    return jax.shard_map(
        body,
        mesh=mesh,
        in_specs=(
            P("lat", "lon", None),
            P("lat", "lon", None, None, None),
            P("lat", "lon", None),
            P("lat", "lon", None, None),
            P("lat", "lon", None, None),
            P("lat", "lon"),
            P("lat", "lon", None),
        ),
        out_specs=P("lat", "lon", None),
        check_vma=False,
    )
```

```python
import functools

import jax
import jax.numpy as jnp
from jax import lax
from jax.experimental import pallas as pl
from jax.experimental.pallas import tpu as pltpu
from jax.sharding import PartitionSpec as P

F32 = jnp.float32
BF16 = jnp.bfloat16
MESH = pl.DeviceIdType.MESH
NSI = 6
LOC = 12
K = 64
OB = 128
CLAT = 8
CLON = 16
NBLK = 32
NNB = 12
LEV = 32
NT = 17
PAD = 33
CHUNKS = ((0, 6), (6, 12), (12, 17))
ORDER = (0, 1, 2, 3, 4, 5, 6, 7, 8, 16, 24, 9, 10, 11, 12, 13, 14, 15) + tuple(range(17, 24)) + tuple(range(25, 32))


def dot(a, b):
    return jnp.dot(a, b, preferred_element_type=F32)


def split(x):
    hi = x.astype(BF16)
    return hi, (x - hi.astype(F32)).astype(BF16)


def diagonal(x, left, right):
    first, second = x[:, :128], x[:, 128:]
    zero = jnp.zeros_like(first)
    return jnp.concatenate(
        [
            jnp.concatenate([first * left, zero], 1),
            jnp.concatenate([first * right, zero], 1),
            jnp.concatenate([zero, second * left], 1),
            jnp.concatenate([zero, second * right], 1),
        ],
        0,
    )


def kernel(
    na, nb, ens_h, w_h, bcol_h, innov_h, prec_h, cnt, nbs_h, out,
    out_v, o_sem, pf, yf, ens, w, bcol, innov, prec, nbs, in_sem, yb, sa, sg, sp, gall, nbp, msend, mrecv, ssend, srecv, own, s2, zf, tb, csend, rrow, rcol, rcor, dd, xa, sx, so,
    scales, g_send, g_recv, n_send, n_recv, m_send, m_recv, s_send, s_recv, t_send, t_recv,
):
    loads = [
        pltpu.make_async_copy(src, dst, in_sem.at[i])
        for i, (src, dst) in enumerate(
            ((bcol_h, bcol), (ens_h, ens), (prec_h, prec), (innov_h, innov), (w_h, w), (nbs_h, nbs))
        )
    ]
    for load in loads:
        load.start()
    ia, jb = lax.axis_index("lat"), lax.axis_index("lon")
    up, down = lax.rem(ia + na - 1, na), lax.rem(ia + 1, na)
    west, east = lax.rem(jb + nb - 1, nb), lax.rem(jb + 1, nb)

    has_up, has_down = ia > 0, ia < na - 1

    barrier = pltpu.get_barrier_semaphore()

    def greet(peers):
        for peer in peers:
            pl.semaphore_signal(barrier, inc=1, device_id=peer, device_id_type=MESH)

    greet(((ia, west), (ia, east)))
    pl.when(has_up)(lambda: greet(((up, jb), (up, west))))
    pl.when(has_down)(lambda: greet(((down, jb), (down, east))))

    @pl.when(jnp.logical_not(has_up))
    def _():
        srecv[0] = jnp.zeros_like(srecv[0])
        nbp[2] = jnp.zeros_like(nbp[2])

    @pl.when(jnp.logical_not(has_down))
    def _():
        srecv[1] = jnp.zeros_like(srecv[1])
        nbp[0] = jnp.zeros_like(nbp[0])
        rrow[...] = jnp.zeros_like(rrow)
        rcor[...] = jnp.zeros_like(rcor)

    def each(cond, copies, what):
        def run():
            for copy in copies:
                getattr(copy, what)()

        pl.when(cond)(run)

    def remote(src, dst, send, recv, peer):
        return pltpu.make_async_remote_copy(
            src_ref=src, dst_ref=dst, send_sem=send, recv_sem=recv, device_id=peer, device_id_type=MESH
        )

    lane1 = lax.broadcasted_iota(jnp.int32, (1, 128), 1)
    left_f = (lane1 < 64).astype(F32)
    left, right = left_f.astype(BF16), (1.0 - left_f).astype(BF16)
    row128 = lax.broadcasted_iota(jnp.int32, (128, 128), 0)
    lane128 = lax.broadcasted_iota(jnp.int32, (128, 128), 1)
    averager = jnp.where(row128 // 64 == lane128 // 64, 1.0 / K, 0.0).astype(BF16)

    loads[0].wait()
    loads[1].wait()

    code = jnp.zeros((1, 128), jnp.int32)
    columns = jnp.concatenate([bcol[...], jnp.zeros((1, 128 - NBLK), jnp.int32)], 1)
    live = (lane1 < cnt[0, 0]) & (lane1 < NBLK)
    code = jnp.where(live, columns + 1, 0)
    msend[0] = jnp.broadcast_to(code, (8, 128))
    msend[1] = jnp.broadcast_to(pltpu.roll(code, 2 * NBLK, 1), (8, 128))
    code_own = pltpu.roll(code, NBLK, 1)

    chosen = jnp.where(row128 == jnp.broadcast_to(columns, (128, 128)), 1.0, 0.0)
    chosen = jnp.where(lane128 < NBLK, chosen, 0.0)
    chosen = jnp.transpose(chosen)[:NBLK].astype(BF16)
    state = ens[...].reshape(CLAT * CLON, LEV * K)
    picked = dot(chosen, state)
    stacked = jnp.concatenate([picked[:, 128 * t : 128 * (t + 1)] for t in range(16)], 0)
    anomaly = stacked - dot(stacked.astype(BF16), averager)
    for t in range(16):
        part = anomaly[NBLK * t : NBLK * (t + 1)]
        sa[pl.ds(2 * t * PAD, NBLK), :] = part
        sa[pl.ds((2 * t + 1) * PAD, NBLK), :] = pltpu.roll(part, 64, 1)
    for load in loads[2:5]:
        load.wait()
    sp[0] = jnp.sqrt(prec[...].astype(F32))
    sp[1] = innov[...].astype(F32) * sp[0]

    U1, U2, REP = 32, 32, 1

    def observed(step, carry):
        for i in range(U1):
            b = lax.rem(step, 32 // U1) * U1 + i
            x = sa[pl.ds(b, LEV, stride=PAD), :][:, :K].astype(BF16)
            y = lax.dot_general(x, w[b], (((0,), (0,)), ((), ())), preferred_element_type=F32)
            yb[b, 0:K] = (y * sp[0, pl.ds(b, 1), :]).astype(BF16)
            forced = sp[1, pl.ds(b, 1), :]
            yb[b, K : K + 16] = jnp.where(lax.broadcasted_iota(jnp.int32, (16, 128), 0) == 0, forced, 0.0).astype(BF16)
        return carry

    def squared(step, carry):
        for i in range(U2):
            b = lax.rem(step, 32 // U2) * U2 + i
            g = lax.dot_general(yb[b], yb[b, 0:K], (((1,), (1,)), ((), ())), preferred_element_type=F32)
            sg[pl.ds(b, 72, stride=PAD), 0:K] = g[:72]
        return carry

    lax.fori_loop(0, 32 // U1 * REP, observed, 0)
    lax.fori_loop(0, 32 // U2 * REP, squared, 0)

    wide = lax.broadcasted_iota(jnp.int32, (NBLK, 128), 1)
    def unit(k):
        return sg[pl.ds(k * PAD, NBLK), :]

    def pack(i):
        if i == 16:
            spine = jnp.zeros((NBLK, 128), F32)
            for k in range(32, 64):
                spine = jnp.where(wide == k, unit(k), spine)
            gall[1, 16] = jnp.where(wide < 64, unit(64), pltpu.roll(spine, 64, 1)).astype(BF16)
            return
        k = i + 16
        low = unit(i) if i == 0 else jnp.where(wide >= i, unit(i), pltpu.roll(unit(63 - i), 64 + i, 1))
        high = jnp.where(wide >= 64 + k, pltpu.roll(unit(k), 64, 1), pltpu.roll(unit(63 - k), k, 1))
        gall[1, i] = jnp.where(wide < 64, low, high).astype(BF16)

    loads[5].wait()
    for to, start, rows in ((0, 0, 8), (8, 8, 1), (9, 16, 1), (10, 24, 1), (11, 9, 7), (18, 17, 7), (25, 25, 7)):
        nbp[1, to : to + rows, 0:NNB] = nbs[start : start + rows]
    pl.semaphore_wait(barrier, 2 + 2 * has_up.astype(jnp.int32) + 2 * has_down.astype(jnp.int32))
    facts = [
        remote(nbp.at[1], nbp.at[0], n_send.at[0], n_recv.at[0], (up, jb)),
        remote(nbp.at[1], nbp.at[2], n_send.at[1], n_recv.at[1], (down, jb)),
        remote(msend.at[0], mrecv.at[0], m_send.at[0], m_recv.at[0], (ia, east)),
        remote(msend.at[1], mrecv.at[1], m_send.at[1], m_recv.at[1], (ia, west)),
    ]
    each(has_up, facts[:1], "start")
    each(has_down, facts[1:2], "start")
    for copy in facts[2:]:
        copy.start()
    for i in range(17):
        pack(i)
    first = []
    for n, (lo, hi) in enumerate(CHUNKS):
        span = pl.ds(lo, hi - lo)
        pair = [
            remote(gall.at[1, span], gall.at[0, span], g_send.at[0, n], g_recv.at[0, n], (ia, east)),
            remote(gall.at[1, span], gall.at[2, span], g_send.at[1, n], g_recv.at[1, n], (ia, west)),
        ]
        for copy in pair:
            copy.start()
        first.append(pair)

    def columns_of(r, carry):
        x = jnp.concatenate([ens[r, :, 128 * t : 128 * (t + 1)] for t in range(16)], 0)
        spread = (x.astype(F32) - dot(x, averager)).astype(BF16).astype(F32)
        for t in range(16):
            sx[r, pl.ds(t * 17, CLON), :] = spread[CLON * t : CLON * (t + 1)]
        for c in range(CLON):
            xa[r * CLON + c] = sx[r, pl.ds(c, 16, stride=17), :].astype(BF16)
        return carry

    lax.fori_loop(0, CLAT, columns_of, 0)

    each(has_down, facts[:1], "wait_recv")
    each(has_up, facts[1:2], "wait_recv")
    for copy in facts[2:]:
        copy.wait_recv()
    code3 = mrecv[0, 0:1, :] + code_own + mrecv[1, 0:1, :]
    is_live = (code3 > 0).astype(F32)
    place = jnp.maximum(code3 - 1, 0)
    b_row = (place // CLON).astype(F32)
    b_col = (place % CLON + (lane1 // NBLK - 1) * CLON).astype(F32)
    point = lax.broadcasted_iota(jnp.int32, (32, 128), 0)
    point = jnp.where(
        point < 8,
        point,
        jnp.where(point < 11, 8 * (point - 7), jnp.where(point < 18, point - 2, jnp.where(point < 25, point - 1, point))),
    )
    p_row = (2 * (point // 8)).astype(F32)
    p_col = (2 * (point % 8)).astype(F32)
    weights = []
    for u in (-1, 0, 1):
        listed = nbp[u + 1]
        count = jnp.zeros((32, 128), F32)
        for n in range(NNB):
            count += (listed[:, n : n + 1] - 96 * (u + 1) == wide).astype(F32)
        dlat = (b_row + float(u * CLAT)) - p_row
        dlon = b_col - p_col
        taper = jnp.exp(-(dlat * dlat + dlon * dlon) / (2.0 * LOC * LOC))
        valid = ((ia - u >= 0) & (ia - u < na)).astype(F32)
        weights.append(jnp.where(wide < 96, count * taper * is_live * valid, 0.0))
    whi, wlo = split(jnp.concatenate(weights, 0))
    lhs = jnp.concatenate([whi, wlo], 0)[:, :96]

    second = []
    for n, (lo, hi) in enumerate(CHUNKS):
        for copy in first[n]:
            copy.wait_recv()
        for t in range(lo, hi, 2):
            ts = range(t, min(t + 2, hi))
            rhs = jnp.concatenate([jnp.concatenate([gall[v, i] for i in ts], 1) for v in range(3)], 0)
            o = dot(lhs, rhs)
            o = o[:96] + o[96:]
            for i in ts:
                part = o[:, 128 * (i - t) : 128 * (i - t + 1)]
                ssend[0, i] = part[:32].astype(BF16)
                own[i] = part[32:64]
                ssend[1, i] = part[64:].astype(BF16)
        span = pl.ds(lo, hi - lo)
        pair = [
            remote(ssend.at[0, span], srecv.at[0, span], s_send.at[0, n], s_recv.at[0, n], (down, jb)),
            remote(ssend.at[1, span], srecv.at[1, span], s_send.at[1, n], s_recv.at[1, n], (up, jb)),
        ]
        each(has_down, pair[:1], "start")
        each(has_up, pair[1:], "start")
        second.append(pair)
    for n, (lo, hi) in enumerate(CHUNKS):
        each(has_up, second[n][:1], "wait_recv")
        each(has_down, second[n][1:], "wait_recv")
        for i in range(lo, hi):
            tile = own[i] + srecv[0, i].astype(F32) + srecv[1, i].astype(F32)
            if i == 16:
                s2[pl.ds(64 * PAD, 32), :] = tile
                s2[pl.ds(65 * PAD, 32), :] = pltpu.roll(tile, 64, 1)
                continue
            k = i + 16
            s2[pl.ds(i * PAD, 32), :] = tile
            s2[pl.ds((63 - i) * PAD, 32), :] = pltpu.roll(tile, 64 - i, 1)
            s2[pl.ds(k * PAD, 32), :] = pltpu.roll(tile, 64, 1)
            s2[pl.ds((63 - k) * PAD, 32), :] = pltpu.roll(tile, 128 - k, 1)
    row64 = lax.broadcasted_iota(jnp.int32, (K, 256), 0)
    lane256 = lax.broadcasted_iota(jnp.int32, (K, 256), 1)
    eye = (lane256 % 64 == row64).astype(F32)
    ones = jnp.where(
        lax.broadcasted_iota(jnp.int32, (256, 256), 0) // 64 == lax.broadcasted_iota(jnp.int32, (256, 256), 1) // 64,
        1.0, 0.0,
    ).astype(BF16)
    half64 = lax.broadcasted_iota(jnp.int32, (K, 128), 1) < 64
    row_k = lax.broadcasted_iota(jnp.int32, (K, 128), 0)
    lane_k = lax.broadcasted_iota(jnp.int32, (K, 128), 1)
    above = (lane_k > row_k) & (lane_k < 64)
    first_diagonal = (lane_k == row_k) & (row_k < 32)
    last_diagonal = (lane_k == row_k) & (row_k >= 32)
    half1 = lane1 < 64
    row16 = lax.broadcasted_iota(jnp.int32, (16, 256), 0)

    def two_rows(x):
        hi = x.astype(BF16).astype(F32)
        return jnp.where(row16 == 0, hi, jnp.where(row16 == 1, x - hi, 0.0)).astype(BF16)

    def both(x):
        return jnp.concatenate(split(x), 0)

    def thrice(a, b_hi, b_lo):
        o = dot(both(a), diagonal(b_hi, left, right))
        return o[:K] + o[K:] + dot(a.astype(BF16), diagonal(b_lo, left, right))

    def symmetric(m):
        upper, own_diagonal = [], []
        for p in (2 * m, 2 * m + 1):
            v = s2[pl.ds(p, K, stride=PAD), :]
            d = jnp.broadcast_to(s2[pl.ds(65 * PAD + p, 1), :], (K, 128))
            upper.append(jnp.where(above, v, 0.0))
            own_diagonal.append(jnp.where(first_diagonal, v, jnp.where(last_diagonal, d, 0.0)))
        whole = jnp.transpose(jnp.concatenate(upper, 0))[:K]
        second_half = pltpu.roll(upper[1] + own_diagonal[1], 64, 1)
        return whole + jnp.where(half64, upper[0] + own_diagonal[0], second_half)

    def begin(g):
        parts, proj = [], []
        for m in (2 * g, 2 * g + 1):
            parts.append(symmetric(m))
            q0 = s2[pl.ds(64 * PAD + 2 * m, 1), :]
            q1 = s2[pl.ds(64 * PAD + 2 * m + 1, 1), :]
            proj.append(jnp.where(half1, q0, pltpu.roll(q1, 64, 1)))
        gram = jnp.concatenate(parts, 1) + (K - 1.0) * eye
        yf[g] = gram
        scales[g, 1:2] = jnp.concatenate(proj, 1)
        scales[g, 0:1] = jnp.sum(gram * gram, axis=0, keepdims=True)

    def first_step(g):
        gram, row = yf[g], scales[g, 1:2]
        sums = dot(two_rows(scales[g, 0:1]), ones)
        g_hi = gram.astype(BF16)
        o = dot(jnp.concatenate([g_hi, two_rows(row)], 0), diagonal(g_hi, left, right))
        inv = 1.0 / jnp.sqrt(sums[0:1] + sums[1:2])
        x = gram * inv
        yf[g] = 1.5 * x - (0.5 * inv * inv) * o[:K]
        zf[g] = 1.5 * eye - 0.5 * x
        scales[g, 0:1] = inv
        scales[g, 1:2] = 1.5 * row - 0.5 * inv * (o[K : K + 1] + o[K + 1 : K + 2])

    def advance(g, refine, keep_y=True):
        y, z, row, p = yf[g], zf[g], scales[g, 1:2], pf[g]
        p_hi, p_lo = split(p)
        top = [y.astype(BF16)] if keep_y else []
        parts = top + [z.astype(BF16), two_rows(row)]
        if refine:
            parts += ([split(y)[1]] if keep_y else []) + [split(z)[1]]
        o = dot(jnp.concatenate(parts, 0), diagonal(p_hi, left, right))
        n = K if keep_y else 0
        yp, zp, rp = o[:n], o[n : n + K], o[n + K : n + K + 1] + o[n + K + 1 : n + K + 2]
        if refine:
            m = n + K + 16
            e = dot(jnp.concatenate(parts[: len(top) + 2], 0), diagonal(p_lo, left, right))
            yp = yp + o[m : m + n] + e[:n]
            zp = zp + o[m + n : m + n + K] + e[n : n + K]
            rp = rp + e[n + K : n + K + 1]
        if keep_y:
            yf[g] = 1.5 * y - 0.5 * yp
        zf[g] = 1.5 * z - 0.5 * zp
        scales[g, 1:2] = 1.5 * row - 0.5 * rp

    def refined(g):
        pf[g] = thrice(zf[g], *split(yf[g]))

    def turn(step, carry):
        for g in range(8):
            pf[g] = dot(zf[g].astype(BF16), diagonal(yf[g].astype(BF16), left, right))
        for g in range(8):
            advance(g, False)
        return carry

    R4, R5 = 1, 1

    def last_turns(groups):
        for g in groups:
            refined(g)
        for g in groups:
            advance(g, R4)
        for g in groups:
            refined(g)
        for g in groups:
            advance(g, R5, False)
        for g in groups:
            z, inv = zf[g], scales[g, 0:1]
            s = dot(both(z * scales[g, 1:2]), ones)
            t = z * (jnp.sqrt(K - 1.0) * jnp.sqrt(inv)) + (s[:K] + s[K:]) * inv
            tb[2 * g] = t[:, :128].astype(BF16)
            tb[2 * g + 1] = t[:, 128:].astype(BF16)

    for g in range(8):
        begin(g)
    for g in range(8):
        first_step(g)
    lax.fori_loop(0, NSI - 3, turn, 0)
    EG = 4
    last_turns(range(EG))

    third = [
        remote(tb.at[pl.ds(0, 4)], rrow, t_send.at[0], t_recv.at[0], (up, jb)),
        remote(csend, rcol, t_send.at[1], t_recv.at[1], (ia, west)),
        remote(tb.at[0], rcor, t_send.at[2], t_recv.at[2], (up, west)),
    ]
    p0, p8, p10 = tb[0].astype(F32), tb[4].astype(F32), tb[5].astype(F32)
    csend[0] = jnp.where(half64, p0, pltpu.roll(p8, 64, 1)).astype(BF16)
    csend[1] = jnp.where(half64, pltpu.roll(p8, 64, 1), pltpu.roll(p10, 64, 1)).astype(BF16)
    third[1].start()
    each(has_up, third[::2], "start")
    last_turns(range(EG, 8))
    zero64 = jnp.zeros((K, 128), F32)

    def expand(pair):
        v = pair.astype(F32)
        r = pltpu.roll(v, 64, 1)
        d0 = jnp.concatenate([jnp.where(half64, v, zero64), jnp.where(half64, zero64, r)], 0)
        d1 = jnp.concatenate([jnp.where(half64, r, zero64), jnp.where(half64, zero64, v)], 0)
        return d0.astype(BF16), d1.astype(BF16)

    for m in range(16):
        for p, d in zip(ORDER[2 * m : 2 * m + 2], expand(tb[m])):
            dd[p // 8, p % 8] = d

    def finish(a):
        none = jnp.zeros((16, 128), BF16)
        for c in range(8):
            base = 2 * a * CLON + 2 * c
            ee, eo = xa[base], xa[base + 1] * 0.5
            oe, oo = xa[base + CLON] * 0.5, xa[base + CLON + 1] * 0.25
            lower = jnp.concatenate([jnp.concatenate([oe, none], 1), jnp.concatenate([oo, oo], 1)], 0)
            upper = jnp.concatenate([jnp.concatenate([ee, none], 1), jnp.concatenate([eo, eo], 1), lower], 0)
            o = dot(upper, dd[a, c : c + 2].reshape(256, 128))
            e = dot(lower, dd[a + 1, c : c + 2].reshape(256, 128))
            so[0, pl.ds(2 * c, 16, stride=17), :] = o[0:16]
            so[0, pl.ds(2 * c + 1, 16, stride=17), :] = o[16:32]
            so[1, pl.ds(2 * c, 16, stride=17), :] = o[32:48] + e[0:16]
            so[1, pl.ds(2 * c + 1, 16, stride=17), :] = o[48:64] + e[16:32]
        for i in range(2):
            r = 2 * a + i
            x = jnp.concatenate([ens[r, :, 128 * t : 128 * (t + 1)] for t in range(16)], 0)
            center = dot(x, averager)
            for t in range(16):
                rows = so[i, pl.ds(t * 17, CLON), :] + center[CLON * t : CLON * (t + 1)]
                out[r, :, 128 * t : 128 * (t + 1)] = rows.astype(BF16)

    def drain(a):
        return pltpu.make_async_copy(out_v.at[pl.ds(2 * a, 2)], out.at[pl.ds(2 * a, 2)], o_sem.at[a])

    third[1].wait_recv()
    for i in range(2):
        for p, d in zip(((0, 1), (2, 3))[i], expand(rcol[i])):
            dd[p, 8] = d

    def most(a, carry):
        finish(a)
        return carry

    lax.fori_loop(0, 3, most, 0)
    each(has_down, third[::2], "wait_recv")
    edge = (ia == na - 1).astype(F32)
    for i in range(4):
        for c, d in zip((2 * i, 2 * i + 1), expand(rrow[i])):
            dd[4, c] = (d.astype(F32) * (1.0 - edge) + dd[3, c].astype(F32) * edge).astype(BF16)
    bottom = pltpu.roll(rcol[1].astype(F32), 64, 1)
    dd[4, 8] = expand(rcor[...].astype(F32) * (1.0 - edge) + bottom * edge)[0]
    finish(3)
    for copy in facts[2:] + third[1:2] + [copy for pair in first for copy in pair]:
        copy.wait_send()
    each(has_up, facts[:1] + third[::2] + [pair[1] for pair in second], "wait_send")
    each(has_down, facts[1:2] + [pair[0] for pair in second], "wait_send")


def solution(mesh):
    na, nb = mesh.shape["lat"], mesh.shape["lon"]

    def body(ensemble, channel_weights, block_column, innovation, error_precision, block_count, neighbours):
        dma = pltpu.SemaphoreType.DMA
        return pl.pallas_call(
            functools.partial(kernel, na, nb),
            out_shape=jax.ShapeDtypeStruct(ensemble.shape, BF16),
            in_specs=[pl.BlockSpec(memory_space=pltpu.SMEM if i == 5 else pltpu.HBM) for i in range(7)],
            out_specs=pl.BlockSpec(memory_space=pltpu.VMEM),
            scratch_shapes=[
                pltpu.VMEM(ensemble.shape, BF16),
                dma((4,)),
                pltpu.VMEM((8, K, 256), F32),
                pltpu.VMEM((8, K, 256), F32),
                pltpu.VMEM(ensemble.shape, BF16),
                pltpu.VMEM((NBLK, LEV, OB), BF16),
                pltpu.VMEM((1, NBLK), jnp.int32),
                pltpu.VMEM((NBLK, OB), BF16),
                pltpu.VMEM((NBLK, OB), BF16),
                pltpu.VMEM((32, NNB), jnp.int32),
                dma((6,)),
                pltpu.VMEM((NBLK, K + 16, OB), BF16),
                pltpu.VMEM((LEV * PAD, 128), F32),
                pltpu.VMEM((72 * PAD, 128), F32),
                pltpu.VMEM((2, NBLK, OB), F32),
                pltpu.VMEM((3, NT, NBLK, 128), BF16),
                pltpu.VMEM((3, 32, 128), jnp.int32),
                pltpu.VMEM((2, 8, 128), jnp.int32),
                pltpu.VMEM((2, 8, 128), jnp.int32),
                pltpu.VMEM((2, NT, 32, 128), BF16),
                pltpu.VMEM((2, NT, 32, 128), BF16),
                pltpu.VMEM((NT, 32, 128), F32),
                pltpu.VMEM((66 * PAD, 128), F32),
                pltpu.VMEM((8, K, 256), F32),
                pltpu.VMEM((16, K, 128), BF16),
                pltpu.VMEM((2, K, 128), BF16),
                pltpu.VMEM((4, K, 128), BF16),
                pltpu.VMEM((2, K, 128), BF16),
                pltpu.VMEM((K, 128), BF16),
                pltpu.VMEM((5, 9, 128, 128), BF16),
                pltpu.VMEM((CLAT * CLON, 16, 128), BF16),
                pltpu.VMEM((CLAT, 272, 128), F32),
                pltpu.VMEM((2, 272, 128), F32),
                pltpu.VMEM((8, 8, 256), F32),
                dma((2, len(CHUNKS))), dma((2, len(CHUNKS))), dma((2,)), dma((2,)), dma((2,)), dma((2,)),
                dma((2, len(CHUNKS))), dma((2, len(CHUNKS))), dma((3,)), dma((3,)),
            ],
            compiler_params=pltpu.CompilerParams(
                collective_id=0, has_side_effects=True, vmem_limit_bytes=20 * 2**20
            ),
        )(
            *(
                x if x.ndim == 2 and x.shape[1] == 1 else pltpu.with_memory_space_constraint(x, pltpu.HBM)
                for x in (
                    ensemble,
                    channel_weights[0, 0],
                    block_column[0],
                    innovation[0, 0],
                    error_precision[0, 0],
                    block_count,
                    neighbours.reshape(32, NNB),
                )
            )
        )

    return jax.shard_map(
        body,
        mesh=mesh,
        in_specs=(
            P("lat", "lon", None),
            P("lat", "lon", None, None, None),
            P("lat", "lon", None),
            P("lat", "lon", None, None),
            P("lat", "lon", None, None),
            P("lat", "lon"),
            P("lat", "lon", None),
        ),
        out_specs=P("lat", "lon", None),
        check_vma=False,
    )
```
